32 devices in a mesh: gx: 4 (over y, core), gy: 2 (over x), gz: 4 (over z).
Axes of the slice: x: 2, y: 2, z: 4, core: 2. Of those that a mesh axis runs over, the one named last changes fastest.
Arguments:
- density: float32 [32, 32, 512], P('gx', 'gy', 'gz'), may hold values from 0.7 to 1.6
- momentum: float32 [32, 32, 512], P('gx', 'gy', 'gz'), may hold values from -7 to 7
- hydrogen: float32 [32, 32, 512], P('gx', 'gy', 'gz'), may hold values from 0.05 to 1.2
- forced_modes: int32 [96, 3], replicated, may hold values from -3 to 3, as said below
Outputs:
- density_rate: float32 [32, 32, 512], P('gx', 'gy', 'gz')
- momentum_rate: float32 [32, 32, 512], P('gx', 'gy', 'gz')
- hydrogen_rate: float32 [32, 32, 512], P('gx', 'gy', 'gz')
The draws below stay inside these ranges and needn't reach their ends.
Inputs may be any that keep to these rules, and one draw needn't show every extreme that they name: `forced_modes`: each row is a wave vector (kx, ky, kz) with 1 <= kx^2 + ky^2 + kz^2 <= 9; the 96 rows are distinct.
All inputs are finite; a program needn't handle non-finite values.
Results may differ from the reference program's by a relative error of at most 0.0003.
Values sent between devices are 32-bit elements; how exact they have to be, the bound alone decides.
No kernel may reach another device: no remote copies, remote signals or barrier semaphores. Data moves between devices by JAX's collectives and lax.ppermute only.
A program may use at most 64 MiB of HBM per device.

```python
import jax
import jax.numpy as jnp
import numpy as np
from jax import lax

KMAX = 3
MODES = 96
NX = 32
NY = 32
NZ = 512


def draw_momentum(key, part):
    keys = jax.random.split(key, 6)
    noise = jnp.clip(0.35 * jax.random.normal(keys[0], (NX, NY, NZ), jnp.float32), -1.4, 1.4)
    amp_low = 0.4
    amp_high = 1.0
    total = noise
    for term in range(4):
        sub = jax.random.split(keys[term + 1], 3)
        wavevec = jax.random.randint(sub[0], (3,), 0, 2).astype(jnp.float32)
        phases = jax.random.uniform(sub[1], (3,), jnp.float32, -jnp.pi, jnp.pi)
        amplitude = jax.random.uniform(sub[2], (), jnp.float32, amp_low, amp_high)
        wave_x = jnp.cos(2.0 * jnp.pi * wavevec[0] * jnp.arange(NX, dtype=jnp.float32) / NX + phases[0])
        wave_y = jnp.cos(2.0 * jnp.pi * wavevec[1] * jnp.arange(NY, dtype=jnp.float32) / NY + phases[1])
        wave_z = jnp.cos(2.0 * jnp.pi * wavevec[2] * jnp.arange(NZ, dtype=jnp.float32) / NZ + phases[2])
        total = total + amplitude * wave_x[:, None, None] * wave_y[None, :, None] * wave_z[None, None, :]
    return total.astype(jnp.float32)


def wave_sheet(key, rows, cols, theta_low, theta_high):
    keys = jax.random.split(key, 3)
    theta = jax.random.uniform(keys[0], (3,), jnp.float32, theta_low, theta_high)
    drift = jax.random.uniform(keys[1], (3,), jnp.float32, -0.2, 0.2)
    phase = jax.random.uniform(keys[2], (3,), jnp.float32, -jnp.pi, jnp.pi)
    across = jnp.arange(rows, dtype=jnp.float32)[:, None]
    along = jnp.arange(cols, dtype=jnp.float32)[None, :]
    total = jnp.zeros((rows, cols), jnp.float32)
    for term in range(3):
        total = total + 0.09 * jnp.cos(theta[term] * along + drift[term] * across + phase[term])
    return total


def draw_hydrogen(key, part):
    keys = jax.random.split(key, 3)
    sheet_y = wave_sheet(keys[0], NX, NY, 0.5, 1.05)
    sheet_z = wave_sheet(keys[1], NX, NZ, 0.5, 1.05)
    rough = jnp.clip(0.02 * jax.random.normal(keys[2], (NX, NY, NZ), jnp.float32), -0.045, 0.045)
    smooth = 0.6 + sheet_y[:, :, None] + sheet_z[:, None, :]
    return (smooth * (1.0 + rough)).astype(jnp.float32)


def draw_forced_modes(key, part):
    grid = np.arange(-3, 4)
    triples = np.stack(np.meshgrid(grid, grid, grid, indexing='ij'), -1).reshape(-1, 3)
    radius = np.sum(triples * triples, axis=1)
    valid = triples[(radius >= 1) & (radius <= 9)].astype(np.int32)
    chosen = jax.random.permutation(key, valid.shape[0])[:MODES]
    return jnp.asarray(valid)[chosen].astype(jnp.int32)


def steps_of(rng, shape, pieces, smallest, high):
    gain = 1.0
    for axis_at, shards_of in pieces:
        heights = jax.random.uniform(jax.random.fold_in(jax.random.fold_in(rng, 6), axis_at), (shards_of,), jnp.float32, smallest / len(pieces), high / len(pieces))
        gain = gain * jnp.repeat(jnp.exp(heights), shape[axis_at] // shards_of).reshape((-1,) + (1,) * (len(shape) - 1 - axis_at))
    return gain


def setup_inputs(seed: int = 0) -> dict:
    streams_of = jax.random.split(jax.random.key(seed), 5)
    density = jnp.clip(0.7 + 0.90000004 * jax.random.uniform(streams_of[0], (NX, NY, NZ), jnp.float32) ** steps_of(streams_of[0], (NX, NY, NZ), ((0, 4), (1, 2), (2, 4)), -0.2, 0.2), 0.7, 1.6)
    momentum = draw_momentum(jax.random.fold_in(streams_of[4], 71), 0)
    hydrogen = draw_hydrogen(jax.random.fold_in(streams_of[4], 71), 0)
    forced_modes = draw_forced_modes(jax.random.fold_in(streams_of[4], 71), 0)
    return dict(density=density, momentum=momentum, hydrogen=hydrogen, forced_modes=forced_modes)


FIRST_COEFFS = (0.8, -0.2, 4.0 / 105.0, -1.0 / 280.0)
SECOND_COEFFS = (1.6, -0.2, 8.0 / 315.0, -1.0 / 560.0)
CENTRE_COEFF = -205.0 / 72.0
VISCOSITY = 0.3
DIFFUSIVITY = 1.5
FORCE_POWER = 0.3
ENERGY_EPS = 1e-6
ACTIVATION = 2.0
HIGHEST = lax.Precision.HIGHEST


def first_diff(field, axis):
    total = jnp.zeros_like(field)
    for offset, weight in enumerate(FIRST_COEFFS, 1):
        total = total + weight * (jnp.roll(field, -offset, axis) - jnp.roll(field, offset, axis))
    return total


def second_diff(field, axis):
    total = CENTRE_COEFF * field
    for offset, weight in enumerate(SECOND_COEFFS, 1):
        total = total + weight * (jnp.roll(field, -offset, axis) + jnp.roll(field, offset, axis))
    return total


def wave_tables(start, local, total):
    position = start + jnp.arange(local, dtype=jnp.int32)
    wavenum = jnp.arange(-KMAX, KMAX + 1, dtype=jnp.int32)
    phase = (wavenum[:, None] * position[None, :]) % total
    angle = (2.0 * jnp.pi / total) * phase.astype(jnp.float32)
    return jnp.cos(angle), jnp.sin(angle)


def reference(density, momentum, hydrogen, forced_modes):
    size_x, size_y, size_z = density.shape
    velocity = momentum / density
    cos_x, sin_x = wave_tables(0, size_x, size_x)
    cos_y, sin_y = wave_tables(0, size_y, size_y)
    cos_z, sin_z = wave_tables(0, size_z, size_z)
    flat = velocity.reshape(size_x * size_y, size_z)
    part_re = jnp.dot(cos_z, flat.T, precision=HIGHEST).reshape(-1, size_x, size_y)
    part_im = jnp.dot(sin_z, flat.T, precision=HIGHEST).reshape(-1, size_x, size_y)
    mid_re = jnp.einsum('axy,by->abx', part_re, cos_y, precision=HIGHEST) - jnp.einsum('axy,by->abx', part_im, sin_y, precision=HIGHEST)
    mid_im = jnp.einsum('axy,by->abx', part_re, sin_y, precision=HIGHEST) + jnp.einsum('axy,by->abx', part_im, cos_y, precision=HIGHEST)
    cube_re = jnp.einsum('abx,cx->cba', mid_re, cos_x, precision=HIGHEST) - jnp.einsum('abx,cx->cba', mid_im, sin_x, precision=HIGHEST)
    cube_im = jnp.einsum('abx,cx->cba', mid_re, sin_x, precision=HIGHEST) + jnp.einsum('abx,cx->cba', mid_im, cos_x, precision=HIGHEST)
    width = 2 * KMAX + 1
    code = (forced_modes[:, 0] + KMAX) * width * width + (forced_modes[:, 1] + KMAX) * width + (forced_modes[:, 2] + KMAX)
    selector = (code[:, None] == jnp.arange(width ** 3, dtype=jnp.int32)[None, :]).astype(jnp.float32)
    ncell = float(size_x * size_y * size_z)
    coef_cos = jnp.dot(selector, cube_re.reshape(-1), precision=HIGHEST) / ncell
    coef_sin = jnp.dot(selector, cube_im.reshape(-1), precision=HIGHEST) / ncell
    energy = jnp.sum(coef_cos * coef_cos + coef_sin * coef_sin)
    spec_re = jnp.dot(selector.T, coef_cos, precision=HIGHEST).reshape(width, width, width)
    spec_im = -jnp.dot(selector.T, coef_sin, precision=HIGHEST).reshape(width, width, width)
    step_re = jnp.einsum('abc,ax->xbc', spec_re, cos_x, precision=HIGHEST) - jnp.einsum('abc,ax->xbc', spec_im, sin_x, precision=HIGHEST)
    step_im = jnp.einsum('abc,ax->xbc', spec_re, sin_x, precision=HIGHEST) + jnp.einsum('abc,ax->xbc', spec_im, cos_x, precision=HIGHEST)
    plane_re = jnp.einsum('xbc,by->xyc', step_re, cos_y, precision=HIGHEST) - jnp.einsum('xbc,by->xyc', step_im, sin_y, precision=HIGHEST)
    plane_im = jnp.einsum('xbc,by->xyc', step_re, sin_y, precision=HIGHEST) + jnp.einsum('xbc,by->xyc', step_im, cos_y, precision=HIGHEST)
    low = 2.0 * (jnp.dot(plane_re.reshape(-1, width), cos_z, precision=HIGHEST) - jnp.dot(plane_im.reshape(-1, width), sin_z, precision=HIGHEST))
    force = FORCE_POWER * low.reshape(size_x, size_y, size_z) / (energy + ENERGY_EPS)
    density_rate = -first_diff(momentum, 0)
    lap_mom = second_diff(momentum, 0) + second_diff(momentum, 1) + second_diff(momentum, 2)
    lap_fuel = second_diff(hydrogen, 0) + second_diff(hydrogen, 1) + second_diff(hydrogen, 2)
    momentum_rate = -first_diff(momentum * velocity + density, 0) + VISCOSITY * lap_mom + density * force
    hydrogen_rate = -first_diff(hydrogen * velocity, 0) + DIFFUSIVITY * lap_fuel - hydrogen * jnp.exp(-ACTIVATION * hydrogen / density)
    return density_rate, momentum_rate, hydrogen_rate
```

```python
import functools
import math

import jax
import jax.numpy as jnp
import numpy as np
from jax import lax
from jax.experimental import pallas as pl
from jax.experimental.pallas import tpu as pltpu
from jax.sharding import PartitionSpec as P

KMAX = 3
HALO = 4
AXES = ("gx", "gy", "gz")

FIRST_COEFFS = (0.8, -0.2, 4.0 / 105.0, -1.0 / 280.0)
SECOND_COEFFS = (1.6, -0.2, 8.0 / 315.0, -1.0 / 560.0)
CENTRE_COEFF = -205.0 / 72.0
VISCOSITY = 0.3
DIFFUSIVITY = 1.5
FORCE_POWER = 0.3
ENERGY_EPS = 1e-06
ACTIVATION = 2.0
HIGHEST = lax.Precision.HIGHEST

HALF_PLANE = [(0, ky) for ky in range(KMAX + 1)] + [
    (kx, ky) for kx in range(1, KMAX + 1) for ky in range(-KMAX, KMAX + 1)
]


def plane_table(local_x, local_y, full_x, full_y):
    x = np.arange(local_x)[:, None]
    y = np.arange(local_y)[None, :]
    table = np.zeros((local_x * local_y, 128), np.float64)
    for lane, (kx, ky) in enumerate(HALF_PLANE):
        angle = 2.0 * np.pi * (kx * x / full_x + ky * y / full_y)
        table[:, lane] = np.cos(angle).reshape(-1)
        table[:, 32 + lane] = np.sin(angle).reshape(-1)
    return table.astype(np.float32)


def line_table(local_z, full_z):
    z = np.arange(local_z)
    table = np.zeros((8, local_z), np.float64)
    for kz in range(KMAX + 1):
        angle = 2.0 * np.pi * kz * z / full_z
        table[kz] = np.cos(angle)
        table[4 + kz] = np.sin(angle)
    return table.astype(np.float32)


def rotation_tables(counts):
    count_x, count_y, count_z = counts
    lane = np.arange(128)
    wave = lane % 32
    kx = np.array([HALF_PLANE[w][0] if w < len(HALF_PLANE) else 0 for w in wave])
    ky = np.array([HALF_PLANE[w][1] if w < len(HALF_PLANE) else 0 for w in wave])
    sign_xy = np.where(lane & 32, 1.0, -1.0)
    sign_z = np.where(lane & 64, 1.0, -1.0)
    plane = np.zeros((count_x, count_y, 2, 4, 128))
    for i in range(count_x):
        for j in range(count_y):
            angle = 2.0 * np.pi * ((kx * i % count_x) / count_x + (ky * j % count_y) / count_y)
            plane[i, j, 0] = np.cos(angle)
            plane[i, j, 1] = np.sin(angle) * sign_xy
    line = np.zeros((count_z, 2, 4, 128))
    for k in range(count_z):
        angle = 2.0 * np.pi * ((np.arange(4) * k) % count_z) / count_z
        line[k, 0] = np.cos(angle)[:, None]
        line[k, 1] = np.sin(angle)[:, None] * sign_z[None, :]
    plane = plane.reshape(count_x * count_y, 2, 4, 128)
    return plane.astype(np.float32), line.astype(np.float32)


def lanes_of(shape):
    return lax.broadcasted_iota(jnp.int32, shape, len(shape) - 1)


def swap32(a):
    bit = (lanes_of(a.shape) & 32) != 0
    return jnp.where(bit, pltpu.roll(a, 32, 1), pltpu.roll(a, 96, 1))


def swap64(a):
    return pltpu.roll(a, 64, 1)


def pre_kernel(slots, d_ref, m_ref, h_ref, plane_ref, line_ref, rot_ref,
               part_ref, low_ref, high_ref, side_ref, depth_ref):
    size_x, size_y, size_z = d_ref.shape
    flat = (m_ref[...] / d_ref[...]).reshape(size_x * size_y, size_z)
    along = lax.dot_general(line_ref[...], flat, (((1,), (1,)), ((), ())), precision=HIGHEST,
                            preferred_element_type=jnp.float32)
    both = jnp.dot(along, plane_ref[...], precision=HIGHEST, preferred_element_type=jnp.float32)
    part = both[0:4] + swap64(both)[4:8]
    part = rot_ref[0] * part + rot_ref[1] * swap32(part)
    part = rot_ref[2] * part + rot_ref[3] * swap64(part)
    part_ref[...] = jnp.broadcast_to(part[None], (slots, 4, 128))
    for index, ref in enumerate((d_ref, m_ref, h_ref)):
        low_ref[index] = ref[0:HALO]
        high_ref[index] = ref[size_x - HALO:size_x]
    lane = lanes_of((size_y, size_z))
    depth = jnp.zeros((size_y, 128), jnp.float32)
    for f, ref in enumerate((m_ref, h_ref)):
        for i in range(size_x):
            plane = ref[i]
            side_ref[f, i, 0:HALO] = plane[0:HALO]
            side_ref[f, i, HALO:] = plane[size_y - HALO:]
            at = HALO * (f * size_x + i)
            half = 2 * HALO * size_x
            first = pltpu.roll(plane, at, 1)
            last = pltpu.roll(plane, (half + at + HALO) % size_z, 1)
            depth = jnp.where((lane >= at) & (lane < at + HALO), first, depth)
            depth = jnp.where((lane >= half + at) & (lane < half + at + HALO), last, depth)
    depth_ref[...] = depth


def stencil_kernel(d_ref, m_ref, h_ref, before_ref, after_ref, side_prev_ref, side_next_ref,
                   depth_prev_ref, depth_next_ref, modes_ref,
                   density_ref, momentum_ref, hydrogen_ref, weight_ref, pad_ref):
    size_x, size_y, size_z = d_ref.shape

    def planes(ref, index):
        return ([before_ref[index, i] for i in range(HALO)] + [ref[i] for i in range(size_x)]
                + [after_ref[index, i] for i in range(HALO)])

    dens, mom, fuel = planes(d_ref, 0), planes(m_ref, 1), planes(h_ref, 2)
    vel = [a / b for a, b in zip(mom, dens)]
    flux = [a * b + c for a, b, c in zip(mom, vel, dens)]
    carried = [a * b for a, b in zip(fuel, vel)]

    def first_diff(rows, at):
        return sum(w * (rows[at + j] - rows[at - j]) for j, w in enumerate(FIRST_COEFFS, 1))

    lane = lanes_of((size_y, size_z))
    half = 2 * HALO * size_x
    depth_prev = depth_prev_ref[...]
    depth_next = depth_next_ref[...]
    for f, ref in enumerate((m_ref, h_ref)):
        for i in range(size_x):
            pad_ref[f, i, 0:8] = side_prev_ref[f, i]
            pad_ref[f, i, 8:8 + size_y] = ref[i]
            pad_ref[f, i, 8 + size_y:] = side_next_ref[f, i]

    def laplacian(f, rows, i):
        at = i + HALO
        here = rows[at]
        total = (3.0 * CENTRE_COEFF) * here
        slot = HALO * (f * size_x + i)
        after = pltpu.roll(depth_next, (size_z - slot) % size_z, 1)
        before = pltpu.roll(depth_prev, (2 * size_z - HALO - half - slot) % size_z, 1)
        for j, w in enumerate(SECOND_COEFFS, 1):
            side = pad_ref[f, i, 8 + j:8 + j + size_y] + pad_ref[f, i, 8 - j:8 - j + size_y]
            up = pltpu.roll(jnp.where(lane < j, after, here), size_z - j, 1)
            down = pltpu.roll(jnp.where(lane >= size_z - j, before, here), j, 1)
            total = total + w * (rows[at + j] + rows[at - j] + side + up + down)
        return total

    for i in range(size_x):
        at = i + HALO
        density_ref[i] = -first_diff(mom, at)
        momentum_ref[i] = VISCOSITY * laplacian(0, mom, i) - first_diff(flux, at)
        hydrogen_ref[i] = (DIFFUSIVITY * laplacian(1, fuel, i) - first_diff(carried, at)
                           - fuel[at] * jnp.exp(-ACTIVATION * fuel[at] / dens[at]))

    modes = modes_ref[...]
    kx, ky, kz = modes[:, 0:1], modes[:, 1:2], modes[:, 2:3]
    flip = jnp.where((kx < 0) | ((kx == 0) & (ky < 0)), -1, 1)
    kx, ky, kz = kx * flip, ky * flip, kz * flip
    width = 2 * KMAX + 1
    wave = jnp.where(kx == 0, ky, KMAX + 1 + (kx - 1) * width + ky + KMAX)
    code = wave + jnp.where(kz < 0, 64, 0)
    count = modes.shape[0]
    table_lane = lanes_of((count, 128))
    hit = (table_lane & 95) == code
    rows = []
    for c in range(4):
        rows.append(jnp.sum(jnp.where(hit & (jnp.abs(kz) == c), 1.0, 0.0), axis=0, keepdims=True))
    weight_ref[...] = jnp.concatenate(rows, 0)


def post_kernel(cells, d_ref, momentum_ref, parts_ref, weight_ref, plane_ref, line_ref, rot_ref, out_ref):
    size_x, size_y, size_z = d_ref.shape
    total = jnp.sum(parts_ref[...], axis=0) * (1.0 / cells)
    lane = lanes_of((4, 128))
    quad = lane // 32
    other = swap32(swap64(total))
    waves = jnp.where(quad == 2, -total, total) + jnp.where(quad == 0, -other, other)
    weight = weight_ref[...]
    coef = weight * waves
    energy = jnp.sum(coef * waves)
    other = swap32(swap64(coef))
    spec = jnp.where(quad == 2, -coef, coef) + jnp.where(quad == 3, -other, other)
    spec = rot_ref[0] * spec - rot_ref[1] * swap32(spec)
    spec = rot_ref[2] * spec - rot_ref[3] * swap64(spec)
    spec = jnp.concatenate([spec, swap64(spec)], 0)
    mid = lax.dot_general(plane_ref[...], spec, (((1,), (1,)), ((), ())), precision=HIGHEST,
                          preferred_element_type=jnp.float32)
    low = 2.0 * jnp.dot(mid, line_ref[...], precision=HIGHEST, preferred_element_type=jnp.float32)
    force = FORCE_POWER * low.reshape(size_x, size_y, size_z) / (energy + ENERGY_EPS)
    out_ref[...] = momentum_ref[...] + d_ref[...] * force


def shift(x, axis, step):
    size = lax.axis_size(axis)
    return lax.ppermute(x, axis, [(i, (i + step) % size) for i in range(size)])


def per_device(density, momentum, hydrogen, forced_modes):
    size_x, size_y, size_z = density.shape
    counts = tuple(lax.axis_size(a) for a in AXES)
    slots = math.prod(counts)
    gather = slots <= 64
    full = tuple(n * c for n, c in zip(density.shape, counts))
    plane = jnp.asarray(plane_table(size_x, size_y, full[0], full[1]))
    line = jnp.asarray(line_table(size_z, full[2]))
    rot_plane, rot_line = rotation_tables(counts)
    place = lax.axis_index("gx") * counts[1] + lax.axis_index("gy")
    rot = jnp.concatenate([
        lax.dynamic_index_in_dim(jnp.asarray(rot_plane), place, 0, keepdims=False),
        lax.dynamic_index_in_dim(jnp.asarray(rot_line), lax.axis_index("gz"), 0, keepdims=False),
    ], 0)
    f32 = jnp.float32
    block = jax.ShapeDtypeStruct(density.shape, f32)
    end = jax.ShapeDtypeStruct((3, HALO, size_y, size_z), f32)
    parts, low, high, side, depth = pl.pallas_call(
        functools.partial(pre_kernel, slots if gather else 1),
        out_shape=(jax.ShapeDtypeStruct((slots if gather else 1, 4, 128), f32), end, end,
                   jax.ShapeDtypeStruct((2, size_x, 2 * HALO, size_z), f32),
                   jax.ShapeDtypeStruct((size_y, 128), f32)),
    )(density, momentum, hydrogen, plane, line, rot)
    if gather:
        parts = lax.all_to_all(parts, AXES, 0, 0)
    else:
        parts = lax.psum(parts, AXES)
    before = shift(high, "gx", 1)
    after = shift(low, "gx", -1)
    side_prev = shift(side, "gy", 1)
    side_next = side_prev if counts[1] == 2 else shift(side, "gy", -1)
    depth_prev = shift(depth, "gz", 1)
    depth_next = depth_prev if counts[2] == 2 else shift(depth, "gz", -1)
    density_rate, momentum_part, hydrogen_rate, weight = pl.pallas_call(
        stencil_kernel,
        out_shape=(block, block, block, jax.ShapeDtypeStruct((4, 128), f32)),
        scratch_shapes=[pltpu.VMEM((2, size_x, 16 + size_y, size_z), f32)],
    )(density, momentum, hydrogen, before, after, side_prev, side_next, depth_prev, depth_next,
      forced_modes)
    momentum_rate = pl.pallas_call(
        functools.partial(post_kernel, float(math.prod(full))), out_shape=block,
    )(density, momentum_part, parts, weight, plane, line, rot)
    return density_rate, momentum_rate, hydrogen_rate


def solution(mesh):
    in_specs = (P("gx", "gy", "gz"), P("gx", "gy", "gz"), P("gx", "gy", "gz"), P())
    out_specs = (P("gx", "gy", "gz"), P("gx", "gy", "gz"), P("gx", "gy", "gz"))
    return jax.shard_map(
        per_device, mesh=mesh, in_specs=in_specs, out_specs=out_specs, check_vma=False
    )
```

```python
import functools
import math

import jax
import jax.numpy as jnp
import numpy as np
from jax import lax
from jax.experimental import pallas as pl
from jax.experimental.pallas import tpu as pltpu
from jax.sharding import PartitionSpec as P

KMAX = 3
HALO = 4
AXES = ("gx", "gy", "gz")

FIRST_COEFFS = (0.8, -0.2, 4.0 / 105.0, -1.0 / 280.0)
SECOND_COEFFS = (1.6, -0.2, 8.0 / 315.0, -1.0 / 560.0)
CENTRE_COEFF = -205.0 / 72.0
VISCOSITY = 0.3
DIFFUSIVITY = 1.5
FORCE_POWER = 0.3
ENERGY_EPS = 1e-06
ACTIVATION = 2.0
HIGHEST = lax.Precision.HIGHEST

HALF_PLANE = [(0, ky) for ky in range(KMAX + 1)] + [
    (kx, ky) for kx in range(1, KMAX + 1) for ky in range(-KMAX, KMAX + 1)
]


def plane_table(local_x, local_y, full_x, full_y):
    x = np.arange(local_x)[:, None]
    y = np.arange(local_y)[None, :]
    table = np.zeros((local_x * local_y, 128), np.float64)
    for lane, (kx, ky) in enumerate(HALF_PLANE):
        angle = 2.0 * np.pi * (kx * x / full_x + ky * y / full_y)
        table[:, lane] = np.cos(angle).reshape(-1)
        table[:, 32 + lane] = np.sin(angle).reshape(-1)
    return table.astype(np.float32)


def line_table(local_z, full_z):
    z = np.arange(local_z)
    table = np.zeros((8, local_z), np.float64)
    for kz in range(KMAX + 1):
        angle = 2.0 * np.pi * kz * z / full_z
        table[kz] = np.cos(angle)
        table[4 + kz] = np.sin(angle)
    return table.astype(np.float32)


def rotation_tables(counts):
    count_x, count_y, count_z = counts
    lane = np.arange(128)
    wave = lane % 32
    kx = np.array([HALF_PLANE[w][0] if w < len(HALF_PLANE) else 0 for w in wave])
    ky = np.array([HALF_PLANE[w][1] if w < len(HALF_PLANE) else 0 for w in wave])
    sign_xy = np.where(lane & 32, 1.0, -1.0)
    sign_z = np.where(lane & 64, 1.0, -1.0)
    plane = np.zeros((count_x, count_y, 2, 4, 128))
    for i in range(count_x):
        for j in range(count_y):
            angle = 2.0 * np.pi * ((kx * i % count_x) / count_x + (ky * j % count_y) / count_y)
            plane[i, j, 0] = np.cos(angle)
            plane[i, j, 1] = np.sin(angle) * sign_xy
    line = np.zeros((count_z, 2, 4, 128))
    for k in range(count_z):
        angle = 2.0 * np.pi * ((np.arange(4) * k) % count_z) / count_z
        line[k, 0] = np.cos(angle)[:, None]
        line[k, 1] = np.sin(angle)[:, None] * sign_z[None, :]
    plane = plane.reshape(count_x * count_y, 2, 4, 128)
    return plane.astype(np.float32), line.astype(np.float32)


def lanes_of(shape):
    return lax.broadcasted_iota(jnp.int32, shape, len(shape) - 1)


def swap32(a):
    bit = (lanes_of(a.shape) & 32) != 0
    return jnp.where(bit, pltpu.roll(a, 32, 1), pltpu.roll(a, 96, 1))


def swap64(a):
    return pltpu.roll(a, 64, 1)


def fetch_all(sources, targets, sems):
    copies = [pltpu.make_async_copy(a, b, sems.at[n])
              for n, (a, b) in enumerate(zip(sources, targets))]
    for copy in copies:
        copy.start()
    return copies


def rotations(plane_ref, line_ref):
    place = lax.axis_index("gx") * lax.axis_size("gy") + lax.axis_index("gy")
    level = lax.axis_index("gz")
    return plane_ref[place, 0], plane_ref[place, 1], line_ref[level, 0], line_ref[level, 1]


def pre_kernel(slots, *refs):
    sources, targets = refs[:8], refs[8:16]
    part_out, low_ref, high_ref, side_ref, depth_ref, part_ref, sems, part_sem = refs[16:]
    copies = fetch_all(sources, targets, sems)
    d_ref, m_ref, plane_ref, line_ref, rot_plane_ref, rot_line_ref, h_ref, _ = targets
    size_x, size_y, size_z = d_ref.shape
    for copy in copies[:6]:
        copy.wait()
    rot = rotations(rot_plane_ref, rot_line_ref)
    flat = (m_ref[...] / d_ref[...]).reshape(size_x * size_y, size_z)
    along = lax.dot_general(line_ref[...], flat, (((1,), (1,)), ((), ())), precision=HIGHEST,
                            preferred_element_type=jnp.float32)
    both = jnp.dot(along, plane_ref[...], precision=HIGHEST, preferred_element_type=jnp.float32)
    part = both[0:4] + swap64(both)[4:8]
    part = rot[0] * part + rot[1] * swap32(part)
    part = rot[2] * part + rot[3] * swap64(part)
    part_ref[...] = jnp.broadcast_to(part[None], (slots, 4, 128))
    send = pltpu.make_async_copy(part_ref, part_out, part_sem)
    send.start()
    for copy in copies[6:]:
        copy.wait()
    for index, ref in enumerate((d_ref, m_ref, h_ref)):
        low_ref[index] = ref[0:HALO]
        high_ref[index] = ref[size_x - HALO:size_x]
    lane = lanes_of((size_y, size_z))
    depth = jnp.zeros((size_y, 128), jnp.float32)
    for f, ref in enumerate((m_ref, h_ref)):
        for i in range(size_x):
            plane = ref[i]
            side_ref[f, i, 0:HALO] = plane[0:HALO]
            side_ref[f, i, HALO:] = plane[size_y - HALO:]
            at = HALO * (f * size_x + i)
            half = 2 * HALO * size_x
            first = pltpu.roll(plane, at, 1)
            last = pltpu.roll(plane, (half + at + HALO) % size_z, 1)
            depth = jnp.where((lane >= at) & (lane < at + HALO), first, depth)
            depth = jnp.where((lane >= half + at) & (lane < half + at + HALO), last, depth)
    depth_ref[...] = depth
    send.wait()


def mode_counts(modes):
    kx, ky, kz = modes[0:1], modes[1:2], modes[2:3]
    flip = jnp.where((kx < 0) | ((kx == 0) & (ky < 0)), -1, 1)
    kx, ky, kz = kx * flip, ky * flip, kz * flip
    width = 2 * KMAX + 1
    wave = jnp.where(kx == 0, ky, KMAX + 1 + (kx - 1) * width + ky + KMAX)
    code = wave + jnp.where(kz < 0, 64, 0)
    count = modes.shape[1]
    row = lax.broadcasted_iota(jnp.int32, (128, count), 0)
    hit = jnp.where((row & 95) == code, 1.0, 0.0)
    level = jnp.where(lax.broadcasted_iota(jnp.int32, (8, count), 0) == jnp.abs(kz), 1.0, 0.0)
    counts = lax.dot_general(level, hit, (((1,), (1,)), ((), ())),
                             preferred_element_type=jnp.float32)
    return counts[0:4]


def stencil_kernel(d_ref, m_ref, h_ref, before_ref, after_ref, side_prev_ref, side_next_ref,
                   modes_ref, density_out, momentum_ref, hydrogen_ref, weight_ref,
                   pad_ref, density_ref, sem):
    size_x, size_y, size_z = d_ref.shape

    def planes(ref, index):
        return ([before_ref[index, i] for i in range(HALO)] + [ref[i] for i in range(size_x)]
                + [after_ref[index, i] for i in range(HALO)])

    dens, mom, fuel = planes(d_ref, 0), planes(m_ref, 1), planes(h_ref, 2)

    def first_diff(rows, at):
        return sum(w * (rows[at + j] - rows[at - j]) for j, w in enumerate(FIRST_COEFFS, 1))

    for i in range(size_x):
        density_ref[i] = -first_diff(mom, i + HALO)
    send = pltpu.make_async_copy(density_ref, density_out, sem)
    send.start()
    vel = [a / b for a, b in zip(mom, dens)]
    flux = [a * b + c for a, b, c in zip(mom, vel, dens)]
    carried = [a * b for a, b in zip(fuel, vel)]
    for f, ref in enumerate((m_ref, h_ref)):
        for i in range(size_x):
            pad_ref[f, i, 0:8] = side_prev_ref[f, i]
            pad_ref[f, i, 8:8 + size_y] = ref[i]
            pad_ref[f, i, 8 + size_y:] = side_next_ref[f, i]

    def second_diffs(f, rows, i):
        at = i + HALO
        total = (3.0 * CENTRE_COEFF) * rows[at]
        for j, w in enumerate(SECOND_COEFFS, 1):
            side = pad_ref[f, i, 8 + j:8 + j + size_y] + pad_ref[f, i, 8 - j:8 - j + size_y]
            total = total + w * (rows[at + j] + rows[at - j] + side)
        return total

    for i in range(size_x):
        at = i + HALO
        momentum_ref[i] = VISCOSITY * second_diffs(0, mom, i) - first_diff(flux, at)
        hydrogen_ref[i] = (DIFFUSIVITY * second_diffs(1, fuel, i) - first_diff(carried, at)
                           - fuel[at] * jnp.exp(-ACTIVATION * fuel[at] / dens[at]))
    weight_ref[...] = mode_counts(modes_ref[...])
    send.wait()


def depth_kernel(m_ref, h_ref, momentum_ref, hydrogen_ref, depth_prev_ref, depth_next_ref,
                 momentum_out, hydrogen_out, buffer_ref, sem):
    size_x, size_y, size_z = m_ref.shape
    lane = lanes_of((size_y, size_z))
    half = 2 * HALO * size_x
    depth_prev = depth_prev_ref[...]
    depth_next = depth_next_ref[...]

    def depth_part(f, ref, i):
        here = ref[i]
        slot = HALO * (f * size_x + i)
        after = pltpu.roll(depth_next, (size_z - slot) % size_z, 1)
        before = pltpu.roll(depth_prev, (2 * size_z - HALO - half - slot) % size_z, 1)
        total = None
        for j, w in enumerate(SECOND_COEFFS, 1):
            up = pltpu.roll(jnp.where(lane < j, after, here), size_z - j, 1)
            down = pltpu.roll(jnp.where(lane >= size_z - j, before, here), j, 1)
            total = w * (up + down) if total is None else total + w * (up + down)
        return total

    for i in range(size_x):
        buffer_ref[i] = hydrogen_ref[i] + DIFFUSIVITY * depth_part(1, h_ref, i)
    send = pltpu.make_async_copy(buffer_ref, hydrogen_out, sem)
    send.start()
    for i in range(size_x):
        momentum_out[i] = momentum_ref[i] + VISCOSITY * depth_part(0, m_ref, i)
    send.wait()


def post_kernel(cells, d_ref, momentum_ref, parts_ref, weight_ref, plane_ref, line_ref,
                rot_plane_ref, rot_line_ref, out_ref):
    size_x, size_y, size_z = d_ref.shape
    rot = rotations(rot_plane_ref, rot_line_ref)
    total = jnp.sum(parts_ref[...], axis=0) * (1.0 / cells)
    quad = lanes_of((4, 128)) // 32
    other = swap32(swap64(total))
    waves = jnp.where(quad == 2, -total, total) + jnp.where(quad == 0, -other, other)
    coef = weight_ref[...] * waves
    energy = jnp.sum(coef * waves)
    other = swap32(swap64(coef))
    spec = jnp.where(quad == 2, -coef, coef) + jnp.where(quad == 3, -other, other)
    spec = rot[0] * spec - rot[1] * swap32(spec)
    spec = rot[2] * spec - rot[3] * swap64(spec)
    spec = jnp.concatenate([spec, swap64(spec)], 0)
    mid = lax.dot_general(plane_ref[...], spec, (((1,), (1,)), ((), ())), precision=HIGHEST,
                          preferred_element_type=jnp.float32)
    low = 2.0 * jnp.dot(mid, line_ref[...], precision=HIGHEST, preferred_element_type=jnp.float32)
    force = FORCE_POWER * low.reshape(size_x, size_y, size_z) / (energy + ENERGY_EPS)
    out_ref[...] = momentum_ref[...] + d_ref[...] * force


VMEM_SPEC = pl.BlockSpec(memory_space=pltpu.VMEM)
ANY_SPEC = pl.BlockSpec(memory_space=pl.ANY)


def in_vmem(*args):
    return [pltpu.with_memory_space_constraint(a, pltpu.VMEM) for a in args]


def shift(x, axis, step):
    size = lax.axis_size(axis)
    return lax.ppermute(x, axis, [(i, (i + step) % size) for i in range(size)])


def per_device(density, momentum, hydrogen, forced_modes):
    size_x, size_y, size_z = density.shape
    counts = tuple(lax.axis_size(a) for a in AXES)
    devices = math.prod(counts)
    gather = devices <= 64
    slots = devices if gather else 1
    full = tuple(n * c for n, c in zip(density.shape, counts))
    plane = jnp.asarray(plane_table(size_x, size_y, full[0], full[1]))
    line = jnp.asarray(line_table(size_z, full[2]))
    rot_plane, rot_line = (jnp.asarray(t) for t in rotation_tables(counts))
    f32 = jnp.float32
    sources = (density, momentum, plane, line, rot_plane, rot_line, hydrogen, forced_modes.T)
    block = jax.ShapeDtypeStruct(density.shape, f32)
    block_vmem = pltpu.VMEM(density.shape, f32)
    end = pltpu.VMEM((3, HALO, size_y, size_z), f32)
    outs = pl.pallas_call(
        functools.partial(pre_kernel, slots),
        in_specs=[ANY_SPEC] * 8,
        out_specs=[VMEM_SPEC] * 8 + [ANY_SPEC] + [VMEM_SPEC] * 4,
        out_shape=[pltpu.VMEM(a.shape, a.dtype) for a in sources] + [
            jax.ShapeDtypeStruct((slots, 4, 128), f32), end, end,
            pltpu.VMEM((2, size_x, 2 * HALO, size_z), f32), pltpu.VMEM((size_y, 128), f32)],
        scratch_shapes=[pltpu.VMEM((slots, 4, 128), f32), pltpu.SemaphoreType.DMA((8,)),
                        pltpu.SemaphoreType.DMA],
    )(*sources)
    density, momentum, plane, line, rot_plane, rot_line, hydrogen, modes = outs[:8]
    parts, low, high, side, depth = outs[8:]
    if gather:
        parts = lax.all_to_all(parts, AXES, 0, 0)
    else:
        parts = lax.psum(parts, AXES)
    depth_prev = shift(depth, "gz", 1)
    depth_next = depth_prev if counts[2] == 2 else shift(depth, "gz", -1)
    before = shift(high, "gx", 1)
    after = shift(low, "gx", -1)
    side_prev = shift(side, "gy", 1)
    side_next = side_prev if counts[1] == 2 else shift(side, "gy", -1)
    density_rate, momentum_part, hydrogen_part, weight = pl.pallas_call(
        stencil_kernel,
        in_specs=[VMEM_SPEC] * 8,
        out_specs=[ANY_SPEC] + [VMEM_SPEC] * 3,
        out_shape=[block, block_vmem, block_vmem, pltpu.VMEM((4, 128), f32)],
        scratch_shapes=[pltpu.VMEM((2, size_x, 16 + size_y, size_z), f32),
                        pltpu.VMEM(block.shape, f32), pltpu.SemaphoreType.DMA],
    )(*in_vmem(density, momentum, hydrogen, before, after, side_prev, side_next, modes))
    momentum_part, hydrogen_rate = pl.pallas_call(
        depth_kernel,
        in_specs=[VMEM_SPEC] * 6,
        out_specs=[VMEM_SPEC, ANY_SPEC],
        out_shape=[block_vmem, block],
        scratch_shapes=[pltpu.VMEM(block.shape, f32), pltpu.SemaphoreType.DMA],
    )(*in_vmem(momentum, hydrogen, momentum_part, hydrogen_part, depth_prev, depth_next))
    momentum_rate = pl.pallas_call(
        functools.partial(post_kernel, float(math.prod(full))),
        in_specs=[VMEM_SPEC] * 8,
        out_shape=block,
    )(*in_vmem(density, momentum_part, parts, weight, plane, line, rot_plane, rot_line))
    return density_rate, momentum_rate, hydrogen_rate


def solution(mesh):
    in_specs = (P("gx", "gy", "gz"), P("gx", "gy", "gz"), P("gx", "gy", "gz"), P())
    out_specs = (P("gx", "gy", "gz"), P("gx", "gy", "gz"), P("gx", "gy", "gz"))
    return jax.shard_map(
        per_device, mesh=mesh, in_specs=in_specs, out_specs=out_specs, check_vma=False
    )
```

```python
import functools
import math

import jax
import jax.numpy as jnp
import numpy as np
from jax import lax
from jax.experimental import pallas as pl
from jax.experimental.pallas import tpu as pltpu
from jax.sharding import PartitionSpec as P


KMAX = 3
HALO = 4
AXES = ("gx", "gy", "gz")

FIRST_COEFFS = (0.8, -0.2, 4.0 / 105.0, -1.0 / 280.0)
SECOND_COEFFS = (1.6, -0.2, 8.0 / 315.0, -1.0 / 560.0)
CENTRE_COEFF = -205.0 / 72.0
VISCOSITY = 0.3
DIFFUSIVITY = 1.5
FORCE_POWER = 0.3
ENERGY_EPS = 1e-06
ACTIVATION = 2.0
HIGHEST = lax.Precision.HIGHEST

HALF_PLANE = [(0, ky) for ky in range(KMAX + 1)] + [
    (kx, ky) for kx in range(1, KMAX + 1) for ky in range(-KMAX, KMAX + 1)
]


def plane_table(local_x, local_y, full_x, full_y):
    x = np.arange(local_x)[:, None]
    y = np.arange(local_y)[None, :]
    table = np.zeros((local_x * local_y, 128), np.float64)
    for lane, (kx, ky) in enumerate(HALF_PLANE):
        angle = 2.0 * np.pi * (kx * x / full_x + ky * y / full_y)
        table[:, lane] = np.cos(angle).reshape(-1)
        table[:, 32 + lane] = np.sin(angle).reshape(-1)
    return table.astype(np.float32)


def line_table(local_z, full_z):
    z = np.arange(local_z)
    table = np.zeros((8, local_z), np.float64)
    for kz in range(KMAX + 1):
        angle = 2.0 * np.pi * kz * z / full_z
        table[kz] = np.cos(angle)
        table[4 + kz] = np.sin(angle)
    return table.astype(np.float32)


def rotation_tables(counts):
    count_x, count_y, count_z = counts
    lane = np.arange(128)
    wave = lane % 32
    kx = np.array([HALF_PLANE[w][0] if w < len(HALF_PLANE) else 0 for w in wave])
    ky = np.array([HALF_PLANE[w][1] if w < len(HALF_PLANE) else 0 for w in wave])
    sign_xy = np.where(lane & 32, 1.0, -1.0)
    sign_z = np.where(lane & 64, 1.0, -1.0)
    plane = np.zeros((count_x, count_y, 2, 4, 128))
    for i in range(count_x):
        for j in range(count_y):
            angle = 2.0 * np.pi * ((kx * i % count_x) / count_x + (ky * j % count_y) / count_y)
            plane[i, j, 0] = np.cos(angle)
            plane[i, j, 1] = np.sin(angle) * sign_xy
    line = np.zeros((count_z, 2, 4, 128))
    for k in range(count_z):
        angle = 2.0 * np.pi * ((np.arange(4) * k) % count_z) / count_z
        line[k, 0] = np.cos(angle)[:, None]
        line[k, 1] = np.sin(angle)[:, None] * sign_z[None, :]
    plane = plane.reshape(count_x * count_y, 2, 4, 128)
    return plane.astype(np.float32), line.astype(np.float32)


def lanes_of(shape):
    return lax.broadcasted_iota(jnp.int32, shape, len(shape) - 1)


def swap32(a):
    bit = (lanes_of(a.shape) & 32) != 0
    return jnp.where(bit, pltpu.roll(a, 32, 1), pltpu.roll(a, 96, 1))


def swap64(a):
    return pltpu.roll(a, 64, 1)


def fetch_all(sources, targets, sems):
    copies = [pltpu.make_async_copy(a, b, sems.at[n])
              for n, (a, b) in enumerate(zip(sources, targets))]
    for copy in copies:
        copy.start()
    return copies


def rotations(plane_ref, line_ref):
    place = lax.axis_index("gx") * lax.axis_size("gy") + lax.axis_index("gy")
    level = lax.axis_index("gz")
    return plane_ref[place, 0], plane_ref[place, 1], line_ref[level, 0], line_ref[level, 1]


def pre_kernel(slots, *refs):
    sources, targets = refs[:8], refs[8:16]
    part_out, low_ref, high_ref, side_ref, depth_ref, part_ref, sems, part_sem = refs[16:]
    copies = fetch_all(sources, targets, sems)
    d_ref, m_ref, plane_ref, line_ref, rot_plane_ref, rot_line_ref, h_ref, _ = targets
    size_x, size_y, size_z = d_ref.shape
    for copy in copies[:6]:
        copy.wait()
    rot = rotations(rot_plane_ref, rot_line_ref)
    flat = (m_ref[...] / d_ref[...]).reshape(size_x * size_y, size_z)
    along = lax.dot_general(line_ref[...], flat, (((1,), (1,)), ((), ())), precision=HIGHEST,
                            preferred_element_type=jnp.float32)
    both = jnp.dot(along, plane_ref[...], precision=HIGHEST, preferred_element_type=jnp.float32)
    part = both[0:4] + swap64(both)[4:8]
    part = rot[0] * part + rot[1] * swap32(part)
    part = rot[2] * part + rot[3] * swap64(part)
    part_ref[...] = jnp.broadcast_to(part[None], (slots, 4, 128))
    send = pltpu.make_async_copy(part_ref, part_out, part_sem)
    send.start()
    for copy in copies[6:]:
        copy.wait()
    for index, ref in enumerate((d_ref, m_ref, h_ref)):
        low_ref[index] = ref[0:HALO]
        high_ref[index] = ref[size_x - HALO:size_x]
    lane = lanes_of((size_y, size_z))
    depth = jnp.zeros((size_y, 128), jnp.float32)
    for f, ref in enumerate((m_ref, h_ref)):
        for i in range(size_x):
            plane = ref[i]
            side_ref[f, i, 0:HALO] = plane[0:HALO]
            side_ref[f, i, HALO:] = plane[size_y - HALO:]
            at = 2 * HALO * (f * size_x + i)
            first = pltpu.roll(plane, at, 1)
            last = pltpu.roll(plane, (at + 2 * HALO) % size_z, 1)
            depth = jnp.where((lane >= at) & (lane < at + HALO), first, depth)
            depth = jnp.where((lane >= at + HALO) & (lane < at + 2 * HALO), last, depth)
    depth_ref[...] = depth
    send.wait()


def mode_counts(modes):
    kx, ky, kz = modes[0:1], modes[1:2], modes[2:3]
    flip = jnp.where((kx < 0) | ((kx == 0) & (ky < 0)), -1, 1)
    kx, ky, kz = kx * flip, ky * flip, kz * flip
    width = 2 * KMAX + 1
    wave = jnp.where(kx == 0, ky, KMAX + 1 + (kx - 1) * width + ky + KMAX)
    code = wave + jnp.where(kz < 0, 64, 0)
    count = modes.shape[1]
    row = lax.broadcasted_iota(jnp.int32, (128, count), 0)
    hit = jnp.where((row & 95) == code, 1.0, 0.0)
    level = jnp.where(lax.broadcasted_iota(jnp.int32, (8, count), 0) == jnp.abs(kz), 1.0, 0.0)
    counts = lax.dot_general(level, hit, (((1,), (1,)), ((), ())),
                             preferred_element_type=jnp.float32)
    return counts[0:4]


def local_kernel(d_ref, m_ref, h_ref, modes_ref, density_ref, momentum_ref, hydrogen_ref,
                 weight_ref, pad_ref):
    size_x, size_y, size_z = d_ref.shape
    dens = [d_ref[i] for i in range(size_x)]
    mom = [m_ref[i] for i in range(size_x)]
    fuel = [h_ref[i] for i in range(size_x)]
    vel = [a / b for a, b in zip(mom, dens)]
    flux = [a * b + c for a, b, c in zip(mom, vel, dens)]
    carried = [a * b for a, b in zip(fuel, vel)]
    blank = jnp.zeros((8, size_z), jnp.float32)
    for f, rows in enumerate((mom, fuel)):
        for i in range(size_x):
            pad_ref[f, i, 0:8] = blank
            pad_ref[f, i, 8:8 + size_y] = rows[i]
            pad_ref[f, i, 8 + size_y:] = blank
    lane = lanes_of((size_y, size_z))

    def first_diff(rows, i):
        total = jnp.zeros((size_y, size_z), jnp.float32)
        for j, w in enumerate(FIRST_COEFFS, 1):
            if i + j < size_x:
                total = total + w * rows[i + j]
            if i - j >= 0:
                total = total - w * rows[i - j]
        return total

    def second_diffs(f, rows, i):
        here = rows[i]
        total = (3.0 * CENTRE_COEFF) * here
        for j, w in enumerate(SECOND_COEFFS, 1):
            pair = pad_ref[f, i, 8 + j:8 + j + size_y] + pad_ref[f, i, 8 - j:8 - j + size_y]
            pair = pair + jnp.where(lane < size_z - j, pltpu.roll(here, size_z - j, 1), 0.0)
            pair = pair + jnp.where(lane >= j, pltpu.roll(here, j, 1), 0.0)
            if i + j < size_x:
                pair = pair + rows[i + j]
            if i - j >= 0:
                pair = pair + rows[i - j]
            total = total + w * pair
        return total

    for i in range(size_x):
        density_ref[i] = -first_diff(mom, i)
        momentum_ref[i] = VISCOSITY * second_diffs(0, mom, i) - first_diff(flux, i)
        hydrogen_ref[i] = (DIFFUSIVITY * second_diffs(1, fuel, i) - first_diff(carried, i)
                           - fuel[i] * jnp.exp(-ACTIVATION * fuel[i] / dens[i]))
    weight_ref[...] = mode_counts(modes_ref[...])


def edge_kernel(density_part, momentum_part, hydrogen_part, before_ref, after_ref, side_prev_ref,
                side_next_ref, density_ref, momentum_ref, hydrogen_ref, pad_ref):
    size_x, size_y, size_z = density_part.shape

    def outside(ref):
        dens, mom, fuel = ([ref[f, p] for p in range(HALO)] for f in range(3))
        vel = [a / b for a, b in zip(mom, dens)]
        flux = [a * b + c for a, b, c in zip(mom, vel, dens)]
        return mom, flux, fuel, [a * b for a, b in zip(fuel, vel)]

    before, after = outside(before_ref), outside(after_ref)
    row = lax.broadcasted_iota(jnp.int32, (8, size_z), 0)
    blank = jnp.zeros((size_y, size_z), jnp.float32)
    for f in range(2):
        for i in range(size_x):
            pad_ref[f, i, 0:8] = jnp.where(row >= HALO, side_prev_ref[f, i], 0.0)
            pad_ref[f, i, 8:8 + size_y] = blank
            pad_ref[f, i, 8 + size_y:] = jnp.where(row < HALO, side_next_ref[f, i], 0.0)

    def side_part(f, i):
        total = None
        for j, w in enumerate(SECOND_COEFFS, 1):
            pair = pad_ref[f, i, 8 + j:8 + j + size_y] + pad_ref[f, i, 8 - j:8 - j + size_y]
            total = w * pair if total is None else total + w * pair
        return total

    for i in range(size_x):
        density = density_part[i]
        momentum = momentum_part[i] + VISCOSITY * side_part(0, i)
        hydrogen = hydrogen_part[i] + DIFFUSIVITY * side_part(1, i)
        for j, (a, b) in enumerate(zip(FIRST_COEFFS, SECOND_COEFFS), 1):
            for near, at, sign in ((before, i - j + HALO, 1.0), (after, i + j - size_x, -1.0)):
                inside = i - j >= 0 if sign > 0 else i + j < size_x
                if inside:
                    continue
                mom, flux, fuel, carried = (rows[at] for rows in near)
                density = density + (sign * a) * mom
                momentum = momentum + (sign * a) * flux + (VISCOSITY * b) * mom
                hydrogen = hydrogen + (sign * a) * carried + (DIFFUSIVITY * b) * fuel
        density_ref[i] = density
        momentum_ref[i] = momentum
        hydrogen_ref[i] = hydrogen


def post_kernel(cells, d_ref, density_ref, momentum_ref, hydrogen_ref, depth_prev_ref,
                depth_next_ref, parts_ref, weight_ref, plane_ref, line_ref, rot_plane_ref,
                rot_line_ref, density_out, momentum_out, hydrogen_out, buffer_ref, sem):
    size_x, size_y, size_z = d_ref.shape
    send_density = pltpu.make_async_copy(density_ref, density_out, sem.at[2])
    send_density.start()
    lane = lanes_of((size_y, size_z))
    spot = lane % HALO
    late = (lane // HALO) % 2 == 1
    edge = jnp.where(late, depth_prev_ref[...], depth_next_ref[...])
    low_side = SECOND_COEFFS[3] * edge
    high_side = low_side
    for j in (3, 2, 1):
        w = SECOND_COEFFS[j - 1]
        low_side = low_side + jnp.where(spot < j, w * pltpu.roll(edge, size_z - HALO + j, 1), 0.0)
        high_side = high_side + jnp.where(
            spot >= HALO - j, w * pltpu.roll(edge, HALO - j, 1), 0.0)
    edge = jnp.where(late, low_side, high_side)
    rim = (lane < HALO) | (lane >= size_z - HALO)

    def depth_part(f, i):
        at = 2 * HALO * (f * size_x + i)
        return jnp.where(rim, pltpu.roll(edge, (2 * size_z - HALO - at) % size_z, 1), 0.0)

    for i in range(size_x):
        buffer_ref[0, i] = hydrogen_ref[i] + DIFFUSIVITY * depth_part(1, i)
    send_hydrogen = pltpu.make_async_copy(buffer_ref.at[0], hydrogen_out, sem.at[0])
    send_hydrogen.start()

    rot = rotations(rot_plane_ref, rot_line_ref)
    total = jnp.sum(parts_ref[...], axis=0) * (1.0 / cells)
    quad = lanes_of((4, 128)) // 32
    other = swap32(swap64(total))
    waves = jnp.where(quad == 2, -total, total) + jnp.where(quad == 0, -other, other)
    coef = weight_ref[...] * waves
    energy = jnp.sum(coef * waves)
    other = swap32(swap64(coef))
    spec = jnp.where(quad == 2, -coef, coef) + jnp.where(quad == 3, -other, other)
    spec = rot[0] * spec - rot[1] * swap32(spec)
    spec = rot[2] * spec - rot[3] * swap64(spec)
    spec = jnp.concatenate([spec, swap64(spec)], 0)
    mid = lax.dot_general(plane_ref[...], spec, (((1,), (1,)), ((), ())), precision=HIGHEST,
                          preferred_element_type=jnp.float32)
    low = 2.0 * jnp.dot(mid, line_ref[...], precision=HIGHEST, preferred_element_type=jnp.float32)
    force = FORCE_POWER * low.reshape(size_x, size_y, size_z) / (energy + ENERGY_EPS)
    for i in range(size_x):
        part = momentum_ref[i] + VISCOSITY * depth_part(0, i)
        buffer_ref[1, i] = part + d_ref[i] * force[i]
    send_momentum = pltpu.make_async_copy(buffer_ref.at[1], momentum_out, sem.at[1])
    send_momentum.start()
    send_density.wait()
    send_hydrogen.wait()
    send_momentum.wait()


VMEM_SPEC = pl.BlockSpec(memory_space=pltpu.VMEM)
ANY_SPEC = pl.BlockSpec(memory_space=pl.ANY)


def in_vmem(*args):
    return [pltpu.with_memory_space_constraint(a, pltpu.VMEM) for a in args]


def shift(x, axis, step):
    size = lax.axis_size(axis)
    return lax.ppermute(x, axis, [(i, (i + step) % size) for i in range(size)])


def per_device(density, momentum, hydrogen, forced_modes):
    size_x, size_y, size_z = density.shape
    counts = tuple(lax.axis_size(a) for a in AXES)
    devices = math.prod(counts)
    gather = devices <= 64
    slots = devices if gather else 1
    full = tuple(n * c for n, c in zip(density.shape, counts))
    plane = jnp.asarray(plane_table(size_x, size_y, full[0], full[1]))
    line = jnp.asarray(line_table(size_z, full[2]))
    rot_plane, rot_line = (jnp.asarray(t) for t in rotation_tables(counts))
    f32 = jnp.float32
    sources = (density, momentum, plane, line, rot_plane, rot_line, hydrogen, forced_modes.T)
    block = jax.ShapeDtypeStruct(density.shape, f32)
    block_vmem = pltpu.VMEM(density.shape, f32)
    end = pltpu.VMEM((3, HALO, size_y, size_z), f32)
    outs = pl.pallas_call(
        functools.partial(pre_kernel, slots),
        in_specs=[ANY_SPEC] * 8,
        out_specs=[VMEM_SPEC] * 8 + [ANY_SPEC] + [VMEM_SPEC] * 4,
        out_shape=[pltpu.VMEM(a.shape, a.dtype) for a in sources] + [
            jax.ShapeDtypeStruct((slots, 4, 128), f32), end, end,
            pltpu.VMEM((2, size_x, 2 * HALO, size_z), f32), pltpu.VMEM((size_y, 128), f32)],
        scratch_shapes=[pltpu.VMEM((slots, 4, 128), f32), pltpu.SemaphoreType.DMA((8,)),
                        pltpu.SemaphoreType.DMA],
    )(*sources)
    density, momentum, plane, line, rot_plane, rot_line, hydrogen, modes = outs[:8]
    parts, low, high, side, depth = outs[8:]
    if gather:
        parts = lax.all_to_all(parts, AXES, 0, 0)
    else:
        parts = lax.psum(parts, AXES)
    depth_next = shift(depth, "gz", -1)
    depth_prev = depth_next if counts[2] == 2 else shift(depth, "gz", 1)
    after = shift(low, "gx", -1)
    before = shift(high, "gx", 1)
    side_next = shift(side, "gy", -1)
    side_prev = side_next if counts[1] == 2 else shift(side, "gy", 1)
    pad = pltpu.VMEM((2, size_x, 16 + size_y, size_z), f32)
    own = pl.pallas_call(
        local_kernel,
        in_specs=[VMEM_SPEC] * 4,
        out_specs=[VMEM_SPEC] * 4,
        out_shape=[block_vmem] * 3 + [pltpu.VMEM((4, 128), f32)],
        scratch_shapes=[pad],
    )(*in_vmem(density, momentum, hydrogen, modes))
    weight = own[3]
    rates = pl.pallas_call(
        edge_kernel,
        in_specs=[VMEM_SPEC] * 7,
        out_specs=[VMEM_SPEC] * 3,
        out_shape=[block_vmem] * 3,
        scratch_shapes=[pad],
    )(*in_vmem(*own[:3], before, after, side_prev, side_next))
    return tuple(pl.pallas_call(
        functools.partial(post_kernel, float(math.prod(full))),
        in_specs=[VMEM_SPEC] * 12,
        out_specs=[ANY_SPEC] * 3,
        out_shape=[block] * 3,
        scratch_shapes=[pltpu.VMEM((2,) + block.shape, f32), pltpu.SemaphoreType.DMA((3,))],
    )(*in_vmem(density, *rates, depth_prev, depth_next, parts, weight, plane, line,
               rot_plane, rot_line)))


def solution(mesh):
    in_specs = (P("gx", "gy", "gz"), P("gx", "gy", "gz"), P("gx", "gy", "gz"), P())
    out_specs = (P("gx", "gy", "gz"), P("gx", "gy", "gz"), P("gx", "gy", "gz"))
    return jax.shard_map(
        per_device, mesh=mesh, in_specs=in_specs, out_specs=out_specs, check_vma=False
    )
```

```python
import functools
import math

import jax
import jax.numpy as jnp
import numpy as np
from jax import lax
from jax.experimental import pallas as pl
from jax.experimental.pallas import tpu as pltpu
from jax.sharding import PartitionSpec as P


KMAX = 3
HALO = 4
AXES = ("gx", "gy", "gz")

FIRST_COEFFS = (0.8, -0.2, 4.0 / 105.0, -1.0 / 280.0)
SECOND_COEFFS = (1.6, -0.2, 8.0 / 315.0, -1.0 / 560.0)
CENTRE_COEFF = -205.0 / 72.0
VISCOSITY = 0.3
DIFFUSIVITY = 1.5
FORCE_POWER = 0.3
ENERGY_EPS = 1e-06
ACTIVATION = 2.0
HIGHEST = lax.Precision.HIGHEST

HALF_PLANE = [(0, ky) for ky in range(KMAX + 1)] + [
    (kx, ky) for kx in range(1, KMAX + 1) for ky in range(-KMAX, KMAX + 1)
]


def plane_tables(local, counts):
    full_x, full_y = local[0] * counts[0], local[1] * counts[1]
    table = np.zeros((counts[0], counts[1], 64, local[0], local[1]), np.float64)
    for i in range(counts[0]):
        for j in range(counts[1]):
            x = (i * local[0] + np.arange(local[0]))[:, None]
            y = (j * local[1] + np.arange(local[1]))[None, :]
            for row, (kx, ky) in enumerate(HALF_PLANE):
                angle = 2.0 * np.pi * ((kx * x % full_x) / full_x + (ky * y % full_y) / full_y)
                table[i, j, row] = np.cos(angle)
                table[i, j, 32 + row] = np.sin(angle)
    return table.reshape(counts[0] * counts[1], 64, -1).astype(np.float32)


def line_tables(local_z, count):
    full_z = local_z * count
    table = np.zeros((count, 8, local_z), np.float64)
    for i in range(count):
        z = i * local_z + np.arange(local_z)
        for kz in range(KMAX + 1):
            angle = 2.0 * np.pi * (kz * z % full_z) / full_z
            table[i, kz] = np.cos(angle)
            table[i, 4 + kz] = np.sin(angle)
    return table.astype(np.float32)


def deep_tables(table):
    pieces = []
    rest = jnp.asarray(table)
    for _ in range(3):
        piece = rest.astype(jnp.bfloat16)
        pieces.append(piece)
        rest = rest - piece.astype(jnp.float32)
    return jnp.concatenate([pieces[n] for n in (0, 1, 2, 0, 1, 0)], 1)


def lanes_of(shape):
    return lax.broadcasted_iota(jnp.int32, shape, len(shape) - 1)


def split(a):
    high = a.astype(jnp.bfloat16).astype(jnp.float32)
    rest = a - high
    mid = rest.astype(jnp.bfloat16).astype(jnp.float32)
    return high, mid, rest - mid


def four_quadrants(plane):
    return jnp.concatenate([plane, plane[32:64], plane[0:32]], 0)


def swap64(a):
    return pltpu.roll(a, 64, 1)


def fetch_all(sources, targets, sems):
    copies = [pltpu.make_async_copy(a, b, sems.at[n])
              for n, (a, b) in enumerate(zip(sources, targets))]
    for copy in copies:
        copy.start()
    return copies


def pre_kernel(slots, *refs):
    sources, targets = list(refs[:7]), list(refs[7:13])
    part_out, low_ref, high_ref, side_ref, depth_ref, line_ref, part_ref, sems, part_sem = refs[13:]
    targets.insert(2, line_ref)
    place = lax.axis_index("gx") * lax.axis_size("gy") + lax.axis_index("gy")
    level = lax.axis_index("gz")
    sources[2:4] = sources[2].at[level], sources[3].at[place]
    sources[5] = sources[5].at[level]
    copies = fetch_all(sources, targets, sems)
    d_ref, m_ref, _, plane_ref, h_ref = targets[:5]
    size_x, size_y, size_z = d_ref.shape
    for copy in copies[:4]:
        copy.wait()
    flat = (m_ref[...] / d_ref[...]).reshape(size_x * size_y, size_z)
    across = (((1,), (1,)), ((), ()))
    along = lax.dot_general(line_ref[...], flat, across, precision=HIGHEST,
                            preferred_element_type=jnp.float32)
    both = lax.dot_general(along, four_quadrants(plane_ref[...]), across, precision=HIGHEST,
                           preferred_element_type=jnp.float32)
    part = jnp.where(lanes_of((4, 128)) < 64, both[0:4], both[4:8])
    part_ref[...] = jnp.broadcast_to(part[None], (slots, 4, 128))
    send = pltpu.make_async_copy(part_ref, part_out, part_sem)
    send.start()
    for copy in copies[4:]:
        copy.wait()
    for index, ref in enumerate((d_ref, m_ref, h_ref)):
        low_ref[index] = ref[0:HALO]
        high_ref[index] = ref[size_x - HALO:size_x]
    lane = lanes_of((size_y, size_z))
    depth = jnp.zeros((size_y, 128), jnp.float32)
    for f, ref in enumerate((m_ref, h_ref)):
        for i in range(size_x):
            plane = ref[i]
            side_ref[f, i, 0:HALO] = plane[0:HALO]
            side_ref[f, i, HALO:] = plane[size_y - HALO:]
            at = 2 * HALO * (f * size_x + i)
            first = pltpu.roll(plane, at, 1)
            last = pltpu.roll(plane, (at + 2 * HALO) % size_z, 1)
            depth = jnp.where((lane >= at) & (lane < at + HALO), first, depth)
            depth = jnp.where((lane >= at + HALO) & (lane < at + 2 * HALO), last, depth)
    depth_ref[...] = depth
    send.wait()


def mode_counts(modes):
    kx, ky, kz = modes[0:1], modes[1:2], modes[2:3]
    flip = jnp.where((kx < 0) | ((kx == 0) & (ky < 0)), -1, 1)
    kx, ky, kz = kx * flip, ky * flip, kz * flip
    width = 2 * KMAX + 1
    wave = jnp.where(kx == 0, ky, KMAX + 1 + (kx - 1) * width + ky + KMAX)
    code = wave + jnp.where(kz < 0, 64, 0)
    count = modes.shape[1]
    row = lax.broadcasted_iota(jnp.int32, (128, count), 0)
    hit = jnp.where((row & 95) == code, 1.0, 0.0)
    level = jnp.where(lax.broadcasted_iota(jnp.int32, (8, count), 0) == jnp.abs(kz), 1.0, 0.0)
    counts = lax.dot_general(level, hit, (((1,), (1,)), ((), ())),
                             preferred_element_type=jnp.float32)
    return counts[0:4]


def local_kernel(d_ref, m_ref, h_ref, modes_ref, density_ref, momentum_ref, hydrogen_ref,
                 weight_ref, pad_ref):
    size_x, size_y, size_z = d_ref.shape
    dens = [d_ref[i] for i in range(size_x)]
    mom = [m_ref[i] for i in range(size_x)]
    fuel = [h_ref[i] for i in range(size_x)]
    vel = [a / b for a, b in zip(mom, dens)]
    flux = [a * b + c for a, b, c in zip(mom, vel, dens)]
    carried = [a * b for a, b in zip(fuel, vel)]
    blank = jnp.zeros((8, size_z), jnp.float32)
    for f, rows in enumerate((mom, fuel)):
        for i in range(size_x):
            pad_ref[f, i, 0:8] = blank
            pad_ref[f, i, 8:8 + size_y] = rows[i]
            pad_ref[f, i, 8 + size_y:] = blank
    lane = lanes_of((size_y, size_z))

    def first_diff(rows, i):
        total = jnp.zeros((size_y, size_z), jnp.float32)
        for j, w in enumerate(FIRST_COEFFS, 1):
            if i + j < size_x:
                total = total + w * rows[i + j]
            if i - j >= 0:
                total = total - w * rows[i - j]
        return total

    def second_diffs(f, rows, i):
        here = rows[i]
        total = (3.0 * CENTRE_COEFF) * here
        for j, w in enumerate(SECOND_COEFFS, 1):
            pair = pad_ref[f, i, 8 + j:8 + j + size_y] + pad_ref[f, i, 8 - j:8 - j + size_y]
            pair = pair + jnp.where(lane < size_z - j, pltpu.roll(here, size_z - j, 1), 0.0)
            pair = pair + jnp.where(lane >= j, pltpu.roll(here, j, 1), 0.0)
            if i + j < size_x:
                pair = pair + rows[i + j]
            if i - j >= 0:
                pair = pair + rows[i - j]
            total = total + w * pair
        return total

    for i in range(size_x):
        density_ref[i] = -first_diff(mom, i)
        momentum_ref[i] = VISCOSITY * second_diffs(0, mom, i) - first_diff(flux, i)
        hydrogen_ref[i] = (DIFFUSIVITY * second_diffs(1, fuel, i) - first_diff(carried, i)
                           - fuel[i] * jnp.exp(-ACTIVATION * fuel[i] / dens[i]))
    weight_ref[...] = mode_counts(modes_ref[...])


def edge_kernel(density_part, momentum_part, hydrogen_part, before_ref, after_ref, side_prev_ref,
                side_next_ref, density_ref, momentum_ref, hydrogen_ref, pad_ref):
    size_x, size_y, size_z = density_part.shape

    def outside(ref):
        dens, mom, fuel = ([ref[f, p] for p in range(HALO)] for f in range(3))
        vel = [a / b for a, b in zip(mom, dens)]
        flux = [a * b + c for a, b, c in zip(mom, vel, dens)]
        return mom, flux, fuel, [a * b for a, b in zip(fuel, vel)]

    before, after = outside(before_ref), outside(after_ref)
    row = lax.broadcasted_iota(jnp.int32, (8, size_z), 0)
    blank = jnp.zeros((size_y, size_z), jnp.float32)
    for f in range(2):
        for i in range(size_x):
            pad_ref[f, i, 0:8] = jnp.where(row >= HALO, side_prev_ref[f, i], 0.0)
            pad_ref[f, i, 8:8 + size_y] = blank
            pad_ref[f, i, 8 + size_y:] = jnp.where(row < HALO, side_next_ref[f, i], 0.0)

    def side_part(f, i):
        total = None
        for j, w in enumerate(SECOND_COEFFS, 1):
            pair = pad_ref[f, i, 8 + j:8 + j + size_y] + pad_ref[f, i, 8 - j:8 - j + size_y]
            total = w * pair if total is None else total + w * pair
        return total

    for i in range(size_x):
        density = density_part[i]
        momentum = momentum_part[i] + VISCOSITY * side_part(0, i)
        hydrogen = hydrogen_part[i] + DIFFUSIVITY * side_part(1, i)
        for j, (a, b) in enumerate(zip(FIRST_COEFFS, SECOND_COEFFS), 1):
            for near, at, sign in ((before, i - j + HALO, 1.0), (after, i + j - size_x, -1.0)):
                inside = i - j >= 0 if sign > 0 else i + j < size_x
                if inside:
                    continue
                mom, flux, fuel, carried = (rows[at] for rows in near)
                density = density + (sign * a) * mom
                momentum = momentum + (sign * a) * flux + (VISCOSITY * b) * mom
                hydrogen = hydrogen + (sign * a) * carried + (DIFFUSIVITY * b) * fuel
        density_ref[i] = density
        momentum_ref[i] = momentum
        hydrogen_ref[i] = hydrogen


def post_kernel(cells, d_ref, density_ref, momentum_ref, hydrogen_ref, depth_prev_ref,
                depth_next_ref, parts_ref, weight_ref, plane_ref, line_ref, density_out,
                momentum_out, hydrogen_out, buffer_ref, sem):
    size_x, size_y, size_z = d_ref.shape
    send_density = pltpu.make_async_copy(density_ref, density_out, sem.at[2])
    send_density.start()
    lane = lanes_of((size_y, size_z))
    spot = lane % HALO
    late = (lane // HALO) % 2 == 1
    edge = jnp.where(late, depth_prev_ref[...], depth_next_ref[...])
    low_side = SECOND_COEFFS[3] * edge
    high_side = low_side
    for j in (3, 2, 1):
        w = SECOND_COEFFS[j - 1]
        low_side = low_side + jnp.where(spot < j, w * pltpu.roll(edge, size_z - HALO + j, 1), 0.0)
        high_side = high_side + jnp.where(
            spot >= HALO - j, w * pltpu.roll(edge, HALO - j, 1), 0.0)
    edge = jnp.where(late, low_side, high_side)
    rim = (lane < HALO) | (lane >= size_z - HALO)

    def depth_part(f, i):
        at = 2 * HALO * (f * size_x + i)
        return jnp.where(rim, pltpu.roll(edge, (2 * size_z - HALO - at) % size_z, 1), 0.0)

    for i in range(size_x):
        buffer_ref[0, i] = hydrogen_ref[i] + DIFFUSIVITY * depth_part(1, i)
    send_hydrogen = pltpu.make_async_copy(buffer_ref.at[0], hydrogen_out, sem.at[0])
    send_hydrogen.start()

    parts = [parts_ref[n] for n in range(parts_ref.shape[0])]
    while len(parts) > 1:
        half = len(parts) // 2
        parts = [a + b for a, b in zip(parts[:half], parts[half:])] + parts[2 * half:]
    total = parts[0] * (1.0 / cells)
    quad = lanes_of((4, 128)) // 32
    other = swap64(total)
    waves = jnp.where(quad == 3, -total, total) + jnp.where(quad == 0, -other, other)
    coef = weight_ref[...] * waves
    energy = jnp.sum(coef * waves)
    other = swap64(coef)
    spec = jnp.where(quad == 3, -coef, coef) + jnp.where(quad == 2, -other, other)
    spec = jnp.concatenate([jnp.where(quad < 2, spec, 0.0), jnp.where(quad < 2, 0.0, spec)], 0)
    mid = jnp.dot(spec, four_quadrants(plane_ref[...]), precision=HIGHEST,
                  preferred_element_type=jnp.float32)
    high, middle, rest = split(mid)
    mid = jnp.concatenate([high, high, high, middle, middle, rest], 0).astype(jnp.bfloat16)
    low = lax.dot_general(mid, line_ref[...], (((0,), (0,)), ((), ())),
                          preferred_element_type=jnp.float32)
    scale = 2.0 * FORCE_POWER / (energy + ENERGY_EPS)
    force = low.reshape(size_x, size_y, size_z) * scale
    for i in range(size_x):
        part = momentum_ref[i] + VISCOSITY * depth_part(0, i)
        buffer_ref[1, i] = part + d_ref[i] * force[i]
    send_momentum = pltpu.make_async_copy(buffer_ref.at[1], momentum_out, sem.at[1])
    send_momentum.start()
    send_density.wait()
    send_hydrogen.wait()
    send_momentum.wait()


VMEM_SPEC = pl.BlockSpec(memory_space=pltpu.VMEM)
ANY_SPEC = pl.BlockSpec(memory_space=pl.ANY)


def in_vmem(*args):
    return [pltpu.with_memory_space_constraint(a, pltpu.VMEM) for a in args]


def shift(x, axis, step):
    size = lax.axis_size(axis)
    return lax.ppermute(x, axis, [(i, (i + step) % size) for i in range(size)])


def per_device(density, momentum, hydrogen, forced_modes):
    size_x, size_y, size_z = density.shape
    counts = tuple(lax.axis_size(a) for a in AXES)
    devices = math.prod(counts)
    gather = devices <= 64
    slots = devices if gather else 1
    full = tuple(n * c for n, c in zip(density.shape, counts))
    plane = jnp.asarray(plane_tables(density.shape, counts))
    line = line_tables(size_z, counts[2])
    deep = deep_tables(line)
    f32 = jnp.float32
    sources = (density, momentum, jnp.asarray(line), plane, hydrogen, deep, forced_modes.T)
    kept = [pltpu.VMEM(a.shape[1:] if n in (3, 5) else a.shape, a.dtype)
            for n, a in enumerate(sources) if n != 2]
    block = jax.ShapeDtypeStruct(density.shape, f32)
    block_vmem = pltpu.VMEM(density.shape, f32)
    end = pltpu.VMEM((3, HALO, size_y, size_z), f32)
    outs = pl.pallas_call(
        functools.partial(pre_kernel, slots),
        in_specs=[ANY_SPEC] * 7,
        out_specs=[VMEM_SPEC] * 6 + [ANY_SPEC] + [VMEM_SPEC] * 4,
        out_shape=kept + [
            jax.ShapeDtypeStruct((slots, 4, 128), f32), end, end,
            pltpu.VMEM((2, size_x, 2 * HALO, size_z), f32), pltpu.VMEM((size_y, 128), f32)],
        scratch_shapes=[pltpu.VMEM(line.shape[1:], f32), pltpu.VMEM((slots, 4, 128), f32),
                        pltpu.SemaphoreType.DMA((7,)),
                        pltpu.SemaphoreType.DMA],
    )(*sources)
    density, momentum, plane, hydrogen, deep, modes = outs[:6]
    parts, low, high, side, depth = outs[6:]
    if gather:
        parts = lax.all_to_all(parts, AXES, 0, 0)
    else:
        parts = lax.psum(parts, AXES)
    depth_next = shift(depth, "gz", -1)
    depth_prev = depth_next if counts[2] == 2 else shift(depth, "gz", 1)
    after = shift(low, "gx", -1)
    before = shift(high, "gx", 1)
    side_next = shift(side, "gy", -1)
    side_prev = side_next if counts[1] == 2 else shift(side, "gy", 1)
    pad = pltpu.VMEM((2, size_x, 16 + size_y, size_z), f32)
    own = pl.pallas_call(
        local_kernel,
        in_specs=[VMEM_SPEC] * 4,
        out_specs=[VMEM_SPEC] * 4,
        out_shape=[block_vmem] * 3 + [pltpu.VMEM((4, 128), f32)],
        scratch_shapes=[pad],
    )(*in_vmem(density, momentum, hydrogen, modes))
    weight = own[3]
    rates = pl.pallas_call(
        edge_kernel,
        in_specs=[VMEM_SPEC] * 7,
        out_specs=[VMEM_SPEC] * 3,
        out_shape=[block_vmem] * 3,
        scratch_shapes=[pad],
    )(*in_vmem(*own[:3], before, after, side_prev, side_next))
    return tuple(pl.pallas_call(
        functools.partial(post_kernel, float(math.prod(full))),
        in_specs=[VMEM_SPEC] * 10,
        out_specs=[ANY_SPEC] * 3,
        out_shape=[block] * 3,
        scratch_shapes=[pltpu.VMEM((2,) + block.shape, f32), pltpu.SemaphoreType.DMA((3,))],
    )(*in_vmem(density, *rates, depth_prev, depth_next, parts, weight, plane, deep)))


def solution(mesh):
    in_specs = (P("gx", "gy", "gz"), P("gx", "gy", "gz"), P("gx", "gy", "gz"), P())
    out_specs = (P("gx", "gy", "gz"), P("gx", "gy", "gz"), P("gx", "gy", "gz"))
    return jax.shard_map(
        per_device, mesh=mesh, in_specs=in_specs, out_specs=out_specs, check_vma=False
    )
```

```python
import functools
import math

import jax
import jax.numpy as jnp
import numpy as np
from jax import lax
from jax.experimental import pallas as pl
from jax.experimental.pallas import tpu as pltpu
from jax.sharding import PartitionSpec as P


KMAX = 3
HALO = 4
AXES = ("gx", "gy", "gz")

FIRST_COEFFS = (0.8, -0.2, 4.0 / 105.0, -1.0 / 280.0)
SECOND_COEFFS = (1.6, -0.2, 8.0 / 315.0, -1.0 / 560.0)
CENTRE_COEFF = -205.0 / 72.0
VISCOSITY = 0.3
DIFFUSIVITY = 1.5
FORCE_POWER = 0.3
ENERGY_EPS = 1e-06
ACTIVATION = 2.0

HALF_PLANE = [(0, ky) for ky in range(KMAX + 1)] + [
    (kx, ky) for kx in range(1, KMAX + 1) for ky in range(-KMAX, KMAX + 1)
]


def plane_tables(local, counts):
    full_x, full_y = local[0] * counts[0], local[1] * counts[1]
    table = np.zeros((counts[0], counts[1], 64, local[0], local[1]), np.float64)
    for i in range(counts[0]):
        for j in range(counts[1]):
            x = (i * local[0] + np.arange(local[0]))[:, None]
            y = (j * local[1] + np.arange(local[1]))[None, :]
            for row, (kx, ky) in enumerate(HALF_PLANE):
                angle = 2.0 * np.pi * ((kx * x % full_x) / full_x + (ky * y % full_y) / full_y)
                table[i, j, row] = np.cos(angle)
                table[i, j, 32 + row] = np.sin(angle)
    return table.reshape(counts[0] * counts[1], 64, -1).astype(np.float32)


def line_tables(local_z, count):
    full_z = local_z * count
    table = np.zeros((count, 8, local_z), np.float64)
    for i in range(count):
        z = i * local_z + np.arange(local_z)
        for kz in range(KMAX + 1):
            angle = 2.0 * np.pi * (kz * z % full_z) / full_z
            table[i, kz] = np.cos(angle)
            table[i, 4 + kz] = np.sin(angle)
    return table.astype(np.float32)


def deep_tables(table):
    pieces = []
    rest = jnp.asarray(table)
    for _ in range(3):
        piece = rest.astype(jnp.bfloat16)
        pieces.append(piece)
        rest = rest - piece.astype(jnp.float32)
    return jnp.concatenate([pieces[n] for n in (0, 1, 2, 0, 1, 0)], 1)


def lanes_of(shape):
    return lax.broadcasted_iota(jnp.int32, shape, len(shape) - 1)


def split(a):
    high = a.astype(jnp.bfloat16).astype(jnp.float32)
    rest = a - high
    mid = rest.astype(jnp.bfloat16).astype(jnp.float32)
    return high, mid, rest - mid


def stacked_rows(a):
    high, mid, low = split(a)
    blank = jnp.zeros_like(a)
    rows = [jnp.concatenate(r, 1) for r in (
        (high, high, high), (mid, mid, blank), (low, blank, blank), (blank, blank, blank))]
    return jnp.concatenate(rows, 0).astype(jnp.bfloat16)


def stacked_columns(a):
    return jnp.concatenate(split(a), 1).astype(jnp.bfloat16)


def fold(a):
    return (a[16:24] + a[8:16]) + a[0:8]


def four_quadrants(plane):
    return jnp.concatenate([plane, plane[32:64], plane[0:32]], 0)


def swap64(a):
    return pltpu.roll(a, 64, 1)


def fetch_all(sources, targets, sems):
    copies = [pltpu.make_async_copy(a, b, sems.at[n])
              for n, (a, b) in enumerate(zip(sources, targets))]
    for n in (2, 3, 0, 1, 4, 5, 6):
        copies[n].start()
    return copies


def pre_kernel(slots, *refs):
    sources, targets = list(refs[:7]), list(refs[7:13])
    part_out, low_ref, high_ref, side_ref, depth_ref, line_ref, part_ref, sems, part_sem = refs[13:]
    targets.insert(2, line_ref)
    place = lax.axis_index("gx") * lax.axis_size("gy") + lax.axis_index("gy")
    level = lax.axis_index("gz")
    sources[2:4] = sources[2].at[level], sources[3].at[place]
    sources[5] = sources[5].at[level]
    copies = fetch_all(sources, targets, sems)
    d_ref, m_ref, _, plane_ref, h_ref = targets[:5]
    size_x, size_y, size_z = d_ref.shape
    across = (((1,), (1,)), ((), ()))
    copies[2].wait()
    copies[3].wait()
    line = stacked_rows(line_ref[...])
    plane = stacked_columns(four_quadrants(plane_ref[...]))
    copies[0].wait()
    copies[1].wait()
    flat = (m_ref[...] / d_ref[...]).reshape(size_x * size_y, size_z)
    along = fold(lax.dot_general(line, stacked_columns(flat), across,
                                 preferred_element_type=jnp.float32))
    both = fold(lax.dot_general(stacked_rows(along), plane, across,
                                preferred_element_type=jnp.float32))
    part = jnp.where(lanes_of((4, 128)) < 64, both[0:4], both[4:8])
    part_ref[...] = jnp.broadcast_to(part[None], (slots, 4, 128))
    send = pltpu.make_async_copy(part_ref, part_out, part_sem)
    send.start()
    for copy in copies[4:]:
        copy.wait()
    for index, ref in enumerate((d_ref, m_ref, h_ref)):
        low_ref[index] = ref[0:HALO]
        high_ref[index] = ref[size_x - HALO:size_x]
    lane = lanes_of((size_y, size_z))
    depth = jnp.zeros((size_y, 128), jnp.float32)
    for f, ref in enumerate((m_ref, h_ref)):
        for i in range(size_x):
            plane = ref[i]
            side_ref[f, i, 0:HALO] = plane[0:HALO]
            side_ref[f, i, HALO:] = plane[size_y - HALO:]
            at = 2 * HALO * (f * size_x + i)
            first = pltpu.roll(plane, at, 1)
            last = pltpu.roll(plane, (at + 2 * HALO) % size_z, 1)
            depth = jnp.where((lane >= at) & (lane < at + HALO), first, depth)
            depth = jnp.where((lane >= at + HALO) & (lane < at + 2 * HALO), last, depth)
    depth_ref[...] = depth
    send.wait()


def mode_counts(modes):
    kx, ky, kz = modes[0:1], modes[1:2], modes[2:3]
    flip = jnp.where((kx < 0) | ((kx == 0) & (ky < 0)), -1, 1)
    kx, ky, kz = kx * flip, ky * flip, kz * flip
    width = 2 * KMAX + 1
    wave = jnp.where(kx == 0, ky, KMAX + 1 + (kx - 1) * width + ky + KMAX)
    code = wave + jnp.where(kz < 0, 64, 0)
    count = modes.shape[1]
    row = lax.broadcasted_iota(jnp.int32, (128, count), 0)
    hit = jnp.where((row & 95) == code, 1.0, 0.0)
    level = jnp.where(lax.broadcasted_iota(jnp.int32, (8, count), 0) == jnp.abs(kz), 1.0, 0.0)
    counts = lax.dot_general(level, hit, (((1,), (1,)), ((), ())),
                             preferred_element_type=jnp.float32)
    return counts[0:4]


def local_kernel(d_ref, m_ref, h_ref, modes_ref, plane_ref, density_ref, momentum_ref,
                 hydrogen_ref, weight_ref, plane_out, pad_ref):
    size_x, size_y, size_z = d_ref.shape
    dens = [d_ref[i] for i in range(size_x)]
    mom = [m_ref[i] for i in range(size_x)]
    fuel = [h_ref[i] for i in range(size_x)]
    vel = [a / b for a, b in zip(mom, dens)]
    flux = [a * b + c for a, b, c in zip(mom, vel, dens)]
    carried = [a * b for a, b in zip(fuel, vel)]
    blank = jnp.zeros((8, size_z), jnp.float32)
    for f, rows in enumerate((mom, fuel)):
        for i in range(size_x):
            pad_ref[f, i, 0:8] = blank
            pad_ref[f, i, 8:8 + size_y] = rows[i]
            pad_ref[f, i, 8 + size_y:] = blank
    lane = lanes_of((size_y, size_z))

    def first_diff(rows, i):
        total = jnp.zeros((size_y, size_z), jnp.float32)
        for j, w in enumerate(FIRST_COEFFS, 1):
            if i + j < size_x:
                total = total + w * rows[i + j]
            if i - j >= 0:
                total = total - w * rows[i - j]
        return total

    def second_diffs(f, rows, i):
        here = rows[i]
        total = (3.0 * CENTRE_COEFF) * here
        for j, w in enumerate(SECOND_COEFFS, 1):
            pair = pad_ref[f, i, 8 + j:8 + j + size_y] + pad_ref[f, i, 8 - j:8 - j + size_y]
            pair = pair + jnp.where(lane < size_z - j, pltpu.roll(here, size_z - j, 1), 0.0)
            pair = pair + jnp.where(lane >= j, pltpu.roll(here, j, 1), 0.0)
            if i + j < size_x:
                pair = pair + rows[i + j]
            if i - j >= 0:
                pair = pair + rows[i - j]
            total = total + w * pair
        return total

    for i in range(size_x):
        density_ref[i] = -first_diff(mom, i)
        momentum_ref[i] = VISCOSITY * second_diffs(0, mom, i) - first_diff(flux, i)
        hydrogen_ref[i] = (DIFFUSIVITY * second_diffs(1, fuel, i) - first_diff(carried, i)
                           - fuel[i] * jnp.exp(-ACTIVATION * fuel[i] / dens[i]))
    weight_ref[...] = mode_counts(modes_ref[...])
    plane_out[...] = jnp.concatenate(
        split(four_quadrants(plane_ref[...])), 0).astype(jnp.bfloat16)


def edge_kernel(density_part, momentum_part, hydrogen_part, before_ref, after_ref, side_prev_ref,
                side_next_ref, density_ref, momentum_ref, hydrogen_ref, pad_ref):
    size_x, size_y, size_z = density_part.shape

    def outside(ref):
        dens, mom, fuel = ([ref[f, p] for p in range(HALO)] for f in range(3))
        vel = [a / b for a, b in zip(mom, dens)]
        flux = [a * b + c for a, b, c in zip(mom, vel, dens)]
        return mom, flux, fuel, [a * b for a, b in zip(fuel, vel)]

    before, after = outside(before_ref), outside(after_ref)
    row = lax.broadcasted_iota(jnp.int32, (8, size_z), 0)
    blank = jnp.zeros((size_y, size_z), jnp.float32)
    for f in range(2):
        for i in range(size_x):
            pad_ref[f, i, 0:8] = jnp.where(row >= HALO, side_prev_ref[f, i], 0.0)
            pad_ref[f, i, 8:8 + size_y] = blank
            pad_ref[f, i, 8 + size_y:] = jnp.where(row < HALO, side_next_ref[f, i], 0.0)

    def side_part(f, i):
        total = None
        for j, w in enumerate(SECOND_COEFFS, 1):
            pair = pad_ref[f, i, 8 + j:8 + j + size_y] + pad_ref[f, i, 8 - j:8 - j + size_y]
            total = w * pair if total is None else total + w * pair
        return total

    for i in range(size_x):
        density = density_part[i]
        momentum = momentum_part[i] + VISCOSITY * side_part(0, i)
        hydrogen = hydrogen_part[i] + DIFFUSIVITY * side_part(1, i)
        for j, (a, b) in enumerate(zip(FIRST_COEFFS, SECOND_COEFFS), 1):
            for near, at, sign in ((before, i - j + HALO, 1.0), (after, i + j - size_x, -1.0)):
                inside = i - j >= 0 if sign > 0 else i + j < size_x
                if inside:
                    continue
                mom, flux, fuel, carried = (rows[at] for rows in near)
                density = density + (sign * a) * mom
                momentum = momentum + (sign * a) * flux + (VISCOSITY * b) * mom
                hydrogen = hydrogen + (sign * a) * carried + (DIFFUSIVITY * b) * fuel
        density_ref[i] = density
        momentum_ref[i] = momentum
        hydrogen_ref[i] = hydrogen


def post_kernel(cells, d_ref, density_ref, momentum_ref, hydrogen_ref, depth_prev_ref,
                depth_next_ref, parts_ref, weight_ref, plane_ref, line_ref, density_out,
                momentum_out, hydrogen_out, buffer_ref, sem):
    size_x, size_y, size_z = d_ref.shape
    send_density = pltpu.make_async_copy(density_ref, density_out, sem.at[2])
    send_density.start()
    lane = lanes_of((size_y, size_z))
    spot = lane % HALO
    late = (lane // HALO) % 2 == 1
    edge = jnp.where(late, depth_prev_ref[...], depth_next_ref[...])
    low_side = SECOND_COEFFS[3] * edge
    high_side = low_side
    for j in (3, 2, 1):
        w = SECOND_COEFFS[j - 1]
        low_side = low_side + jnp.where(spot < j, w * pltpu.roll(edge, size_z - HALO + j, 1), 0.0)
        high_side = high_side + jnp.where(
            spot >= HALO - j, w * pltpu.roll(edge, HALO - j, 1), 0.0)
    edge = jnp.where(late, low_side, high_side)
    rim = (lane < HALO) | (lane >= size_z - HALO)

    def depth_part(f, i):
        at = 2 * HALO * (f * size_x + i)
        return jnp.where(rim, pltpu.roll(edge, (2 * size_z - HALO - at) % size_z, 1), 0.0)

    for i in range(size_x):
        buffer_ref[0, i] = hydrogen_ref[i] + DIFFUSIVITY * depth_part(1, i)
    send_hydrogen = pltpu.make_async_copy(buffer_ref.at[0], hydrogen_out, sem.at[0])
    send_hydrogen.start()

    parts = [parts_ref[n] for n in range(parts_ref.shape[0])]
    while len(parts) > 1:
        half = len(parts) // 2
        parts = [a + b for a, b in zip(parts[:half], parts[half:])] + parts[2 * half:]
    total = parts[0] * (1.0 / cells)
    quad = lanes_of((4, 128)) // 32
    other = swap64(total)
    waves = jnp.where(quad == 3, -total, total) + jnp.where(quad == 0, -other, other)
    coef = weight_ref[...] * waves
    energy = jnp.sum(coef * waves)
    other = swap64(coef)
    spec = jnp.where(quad == 3, -coef, coef) + jnp.where(quad == 2, -other, other)
    spec = jnp.concatenate([jnp.where(quad < 2, spec, 0.0), jnp.where(quad < 2, 0.0, spec)], 0)
    mid = fold(jnp.dot(stacked_rows(spec), plane_ref[...], preferred_element_type=jnp.float32))
    high, middle, rest = split(mid)
    mid = jnp.concatenate([high, high, high, middle, middle, rest], 0).astype(jnp.bfloat16)
    low = lax.dot_general(mid, line_ref[...], (((0,), (0,)), ((), ())),
                          preferred_element_type=jnp.float32)
    scale = 2.0 * FORCE_POWER / (energy + ENERGY_EPS)
    force = low.reshape(size_x, size_y, size_z) * scale
    for i in range(size_x):
        part = momentum_ref[i] + VISCOSITY * depth_part(0, i)
        buffer_ref[1, i] = part + d_ref[i] * force[i]
    send_momentum = pltpu.make_async_copy(buffer_ref.at[1], momentum_out, sem.at[1])
    send_momentum.start()
    send_density.wait()
    send_hydrogen.wait()
    send_momentum.wait()


VMEM_SPEC = pl.BlockSpec(memory_space=pltpu.VMEM)
ANY_SPEC = pl.BlockSpec(memory_space=pl.ANY)


def in_vmem(*args):
    return [pltpu.with_memory_space_constraint(a, pltpu.VMEM) for a in args]


def shift(x, axis, step):
    size = lax.axis_size(axis)
    return lax.ppermute(x, axis, [(i, (i + step) % size) for i in range(size)])


def per_device(density, momentum, hydrogen, forced_modes):
    size_x, size_y, size_z = density.shape
    counts = tuple(lax.axis_size(a) for a in AXES)
    devices = math.prod(counts)
    gather = devices <= 64
    slots = devices if gather else 1
    full = tuple(n * c for n, c in zip(density.shape, counts))
    plane = jnp.asarray(plane_tables(density.shape, counts))
    line = line_tables(size_z, counts[2])
    deep = deep_tables(line)
    f32 = jnp.float32
    sources = (density, momentum, jnp.asarray(line), plane, hydrogen, deep, forced_modes.T)
    kept = [pltpu.VMEM(a.shape[1:] if n in (3, 5) else a.shape, a.dtype)
            for n, a in enumerate(sources) if n != 2]
    block = jax.ShapeDtypeStruct(density.shape, f32)
    block_vmem = pltpu.VMEM(density.shape, f32)
    end = pltpu.VMEM((3, HALO, size_y, size_z), f32)
    outs = pl.pallas_call(
        functools.partial(pre_kernel, slots),
        in_specs=[ANY_SPEC] * 7,
        out_specs=[VMEM_SPEC] * 6 + [ANY_SPEC] + [VMEM_SPEC] * 4,
        out_shape=kept + [
            jax.ShapeDtypeStruct((slots, 4, 128), f32), end, end,
            pltpu.VMEM((2, size_x, 2 * HALO, size_z), f32), pltpu.VMEM((size_y, 128), f32)],
        scratch_shapes=[pltpu.VMEM(line.shape[1:], f32), pltpu.VMEM((slots, 4, 128), f32),
                        pltpu.SemaphoreType.DMA((7,)),
                        pltpu.SemaphoreType.DMA],
    )(*sources)
    density, momentum, plane, hydrogen, deep, modes = outs[:6]
    parts, low, high, side, depth = outs[6:]
    if gather:
        parts = lax.all_to_all(parts, AXES, 0, 0)
    else:
        parts = lax.psum(parts, AXES)
    depth_next = shift(depth, "gz", -1)
    depth_prev = depth_next if counts[2] == 2 else shift(depth, "gz", 1)
    after = shift(low, "gx", -1)
    before = shift(high, "gx", 1)
    side_next = shift(side, "gy", -1)
    side_prev = side_next if counts[1] == 2 else shift(side, "gy", 1)
    pad = pltpu.VMEM((2, size_x, 16 + size_y, size_z), f32)
    own = pl.pallas_call(
        local_kernel,
        in_specs=[VMEM_SPEC] * 5,
        out_specs=[VMEM_SPEC] * 5,
        out_shape=[block_vmem] * 3 + [pltpu.VMEM((4, 128), f32),
                                      pltpu.VMEM((384, size_x * size_y), jnp.bfloat16)],
        scratch_shapes=[pad],
    )(*in_vmem(density, momentum, hydrogen, modes, plane))
    weight, plane = own[3:]
    rates = pl.pallas_call(
        edge_kernel,
        in_specs=[VMEM_SPEC] * 7,
        out_specs=[VMEM_SPEC] * 3,
        out_shape=[block_vmem] * 3,
        scratch_shapes=[pad],
    )(*in_vmem(*own[:3], before, after, side_prev, side_next))
    return tuple(pl.pallas_call(
        functools.partial(post_kernel, float(math.prod(full))),
        in_specs=[VMEM_SPEC] * 10,
        out_specs=[ANY_SPEC] * 3,
        out_shape=[block] * 3,
        scratch_shapes=[pltpu.VMEM((2,) + block.shape, f32), pltpu.SemaphoreType.DMA((3,))],
    )(*in_vmem(density, *rates, depth_prev, depth_next, parts, weight, plane, deep)))


def solution(mesh):
    in_specs = (P("gx", "gy", "gz"), P("gx", "gy", "gz"), P("gx", "gy", "gz"), P())
    out_specs = (P("gx", "gy", "gz"), P("gx", "gy", "gz"), P("gx", "gy", "gz"))
    return jax.shard_map(
        per_device, mesh=mesh, in_specs=in_specs, out_specs=out_specs, check_vma=False
    )
```

```python
import functools
import math

import jax
import jax.numpy as jnp
import numpy as np
from jax import lax
from jax.experimental import pallas as pl
from jax.experimental.pallas import tpu as pltpu
from jax.sharding import PartitionSpec as P


KMAX = 3
HALO = 4
AXES = ("gx", "gy", "gz")

FIRST_COEFFS = (0.8, -0.2, 4.0 / 105.0, -1.0 / 280.0)
SECOND_COEFFS = (1.6, -0.2, 8.0 / 315.0, -1.0 / 560.0)
CENTRE_COEFF = -205.0 / 72.0
VISCOSITY = 0.3
DIFFUSIVITY = 1.5
FORCE_POWER = 0.3
ENERGY_EPS = 1e-06
ACTIVATION = 2.0

HALF_PLANE = [(0, ky) for ky in range(KMAX + 1)] + [
    (kx, ky) for kx in range(1, KMAX + 1) for ky in range(-KMAX, KMAX + 1)
]


def plane_tables(local, counts):
    full_x, full_y = local[0] * counts[0], local[1] * counts[1]
    table = np.zeros((counts[0], counts[1], 64, local[0], local[1]), np.float64)
    for i in range(counts[0]):
        for j in range(counts[1]):
            x = (i * local[0] + np.arange(local[0]))[:, None]
            y = (j * local[1] + np.arange(local[1]))[None, :]
            for row, (kx, ky) in enumerate(HALF_PLANE):
                angle = 2.0 * np.pi * ((kx * x % full_x) / full_x + (ky * y % full_y) / full_y)
                table[i, j, row] = np.cos(angle)
                table[i, j, 32 + row] = np.sin(angle)
    return table.reshape(counts[0] * counts[1], 64, -1).astype(np.float32)


def line_tables(local_z, count):
    full_z = local_z * count
    table = np.zeros((count, 8, local_z), np.float64)
    for i in range(count):
        z = i * local_z + np.arange(local_z)
        for kz in range(KMAX + 1):
            angle = 2.0 * np.pi * (kz * z % full_z) / full_z
            table[i, kz] = np.cos(angle)
            table[i, 4 + kz] = np.sin(angle)
    return table.astype(np.float32)


def deep_tables(table):
    pieces = []
    rest = jnp.asarray(table)
    for _ in range(3):
        piece = rest.astype(jnp.bfloat16)
        pieces.append(piece)
        rest = rest - piece.astype(jnp.float32)
    return jnp.concatenate([pieces[n] for n in (0, 1, 2, 0, 1, 0)], 1)


def lanes_of(shape):
    return lax.broadcasted_iota(jnp.int32, shape, len(shape) - 1)


def split(a):
    high = a.astype(jnp.bfloat16).astype(jnp.float32)
    rest = a - high
    mid = rest.astype(jnp.bfloat16).astype(jnp.float32)
    return high, mid, rest - mid


def stacked_rows(a):
    high, mid, low = split(a)
    blank = jnp.zeros_like(a)
    rows = [jnp.concatenate(r, 1) for r in (
        (high, high, high), (mid, mid, blank), (low, blank, blank), (blank, blank, blank))]
    return jnp.concatenate(rows, 0).astype(jnp.bfloat16)


def stacked_columns(a):
    return jnp.concatenate(split(a), 1).astype(jnp.bfloat16)


def fold(a):
    return (a[16:24] + a[8:16]) + a[0:8]


def four_quadrants(plane):
    return jnp.concatenate([plane, plane[32:64], plane[0:32]], 0)


def swap64(a):
    return pltpu.roll(a, 64, 1)


def fetch_all(sources, targets, sems):
    copies = [pltpu.make_async_copy(a, b, sems.at[n])
              for n, (a, b) in enumerate(zip(sources, targets))]
    for n in (0, 1, 2, 3, 4, 5, 6):
        copies[n].start()
    return copies


def pre_kernel(slots, *refs):
    sources, targets = list(refs[:7]), list(refs[7:13])
    part_out, low_ref, high_ref, side_ref, depth_ref, line_ref, part_ref, sems, part_sem = refs[13:]
    targets.insert(2, line_ref)
    place = lax.axis_index("gx") * lax.axis_size("gy") + lax.axis_index("gy")
    level = lax.axis_index("gz")
    sources[2:4] = sources[2].at[level], sources[3].at[place]
    sources[5] = sources[5].at[level]
    copies = fetch_all(sources, targets, sems)
    d_ref, m_ref, _, plane_ref, h_ref = targets[:5]
    size_x, size_y, size_z = d_ref.shape
    across = (((1,), (1,)), ((), ()))
    copies[2].wait()
    copies[3].wait()
    line = stacked_rows(line_ref[...])
    plane = stacked_columns(four_quadrants(plane_ref[...]))
    copies[0].wait()
    copies[1].wait()
    flat = (m_ref[...] / d_ref[...]).reshape(size_x * size_y, size_z)
    along = fold(lax.dot_general(line, stacked_columns(flat), across,
                                 preferred_element_type=jnp.float32))
    both = fold(lax.dot_general(stacked_rows(along), plane, across,
                                preferred_element_type=jnp.float32))
    part = jnp.where(lanes_of((4, 128)) < 64, both[0:4], both[4:8])
    part_ref[...] = jnp.broadcast_to(part[None], (slots, 4, 128))
    send = pltpu.make_async_copy(part_ref, part_out, part_sem)
    send.start()
    for copy in copies[4:]:
        copy.wait()
    for index, ref in enumerate((d_ref, m_ref, h_ref)):
        low_ref[index] = ref[0:HALO]
        high_ref[index] = ref[size_x - HALO:size_x]
    lane = lanes_of((size_y, size_z))
    depth = jnp.zeros((size_y, 128), jnp.float32)
    for f, ref in enumerate((m_ref, h_ref)):
        for i in range(size_x):
            plane = ref[i]
            side_ref[f, i, 0:HALO] = plane[0:HALO]
            side_ref[f, i, HALO:] = plane[size_y - HALO:]
            at = 2 * HALO * (f * size_x + i)
            first = pltpu.roll(plane, at, 1)
            last = pltpu.roll(plane, (at + 2 * HALO) % size_z, 1)
            depth = jnp.where((lane >= at) & (lane < at + HALO), first, depth)
            depth = jnp.where((lane >= at + HALO) & (lane < at + 2 * HALO), last, depth)
    depth_ref[...] = depth
    send.wait()


def mode_counts(modes):
    kx, ky, kz = modes[0:1], modes[1:2], modes[2:3]
    flip = jnp.where((kx < 0) | ((kx == 0) & (ky < 0)), -1, 1)
    kx, ky, kz = kx * flip, ky * flip, kz * flip
    width = 2 * KMAX + 1
    wave = jnp.where(kx == 0, ky, KMAX + 1 + (kx - 1) * width + ky + KMAX)
    code = wave + jnp.where(kz < 0, 64, 0)
    count = modes.shape[1]
    row = lax.broadcasted_iota(jnp.int32, (128, count), 0)
    hit = jnp.where((row & 95) == code, 1.0, 0.0)
    level = jnp.where(lax.broadcasted_iota(jnp.int32, (8, count), 0) == jnp.abs(kz), 1.0, 0.0)
    counts = lax.dot_general(level, hit, (((1,), (1,)), ((), ())),
                             preferred_element_type=jnp.float32)
    return counts[0:4]


def local_kernel(d_ref, m_ref, h_ref, modes_ref, plane_ref, density_ref, momentum_ref,
                 hydrogen_ref, weight_ref, plane_out, pad_ref):
    size_x, size_y, size_z = d_ref.shape
    dens = [d_ref[i] for i in range(size_x)]
    mom = [m_ref[i] for i in range(size_x)]
    fuel = [h_ref[i] for i in range(size_x)]
    vel = [a / b for a, b in zip(mom, dens)]
    flux = [a * b + c for a, b, c in zip(mom, vel, dens)]
    carried = [a * b for a, b in zip(fuel, vel)]
    blank = jnp.zeros((8, size_z), jnp.float32)
    for f, rows in enumerate((mom, fuel)):
        for i in range(size_x):
            pad_ref[f, i, 0:8] = blank
            pad_ref[f, i, 8:8 + size_y] = rows[i]
            pad_ref[f, i, 8 + size_y:] = blank
    lane = lanes_of((size_y, size_z))

    def first_diff(rows, i):
        total = jnp.zeros((size_y, size_z), jnp.float32)
        for j, w in enumerate(FIRST_COEFFS, 1):
            if i + j < size_x:
                total = total + w * rows[i + j]
            if i - j >= 0:
                total = total - w * rows[i - j]
        return total

    def second_diffs(f, rows, i):
        here = rows[i]
        total = (3.0 * CENTRE_COEFF) * here
        for j, w in enumerate(SECOND_COEFFS, 1):
            pair = pad_ref[f, i, 8 + j:8 + j + size_y] + pad_ref[f, i, 8 - j:8 - j + size_y]
            pair = pair + jnp.where(lane < size_z - j, pltpu.roll(here, size_z - j, 1), 0.0)
            pair = pair + jnp.where(lane >= j, pltpu.roll(here, j, 1), 0.0)
            if i + j < size_x:
                pair = pair + rows[i + j]
            if i - j >= 0:
                pair = pair + rows[i - j]
            total = total + w * pair
        return total

    for i in range(size_x):
        density_ref[i] = -first_diff(mom, i)
        momentum_ref[i] = VISCOSITY * second_diffs(0, mom, i) - first_diff(flux, i)
        hydrogen_ref[i] = (DIFFUSIVITY * second_diffs(1, fuel, i) - first_diff(carried, i)
                           - fuel[i] * jnp.exp(-ACTIVATION * fuel[i] / dens[i]))
    weight_ref[...] = mode_counts(modes_ref[...])
    plane_out[...] = jnp.concatenate(
        split(four_quadrants(plane_ref[...])), 0).astype(jnp.bfloat16)


def edge_kernel(density_part, momentum_part, hydrogen_part, before_ref, after_ref, side_prev_ref,
                side_next_ref, density_ref, momentum_ref, hydrogen_ref, pad_ref):
    size_x, size_y, size_z = density_part.shape

    def outside(ref):
        dens, mom, fuel = ([ref[f, p] for p in range(HALO)] for f in range(3))
        vel = [a / b for a, b in zip(mom, dens)]
        flux = [a * b + c for a, b, c in zip(mom, vel, dens)]
        return mom, flux, fuel, [a * b for a, b in zip(fuel, vel)]

    before, after = outside(before_ref), outside(after_ref)
    row = lax.broadcasted_iota(jnp.int32, (8, size_z), 0)
    blank = jnp.zeros((size_y, size_z), jnp.float32)
    for f in range(2):
        for i in range(size_x):
            pad_ref[f, i, 0:8] = jnp.where(row >= HALO, side_prev_ref[f, i], 0.0)
            pad_ref[f, i, 8:8 + size_y] = blank
            pad_ref[f, i, 8 + size_y:] = jnp.where(row < HALO, side_next_ref[f, i], 0.0)

    def side_part(f, i):
        total = None
        for j, w in enumerate(SECOND_COEFFS, 1):
            pair = pad_ref[f, i, 8 + j:8 + j + size_y] + pad_ref[f, i, 8 - j:8 - j + size_y]
            total = w * pair if total is None else total + w * pair
        return total

    for i in range(size_x):
        density = density_part[i]
        momentum = momentum_part[i] + VISCOSITY * side_part(0, i)
        hydrogen = hydrogen_part[i] + DIFFUSIVITY * side_part(1, i)
        for j, (a, b) in enumerate(zip(FIRST_COEFFS, SECOND_COEFFS), 1):
            for near, at, sign in ((before, i - j + HALO, 1.0), (after, i + j - size_x, -1.0)):
                inside = i - j >= 0 if sign > 0 else i + j < size_x
                if inside:
                    continue
                mom, flux, fuel, carried = (rows[at] for rows in near)
                density = density + (sign * a) * mom
                momentum = momentum + (sign * a) * flux + (VISCOSITY * b) * mom
                hydrogen = hydrogen + (sign * a) * carried + (DIFFUSIVITY * b) * fuel
        density_ref[i] = density
        momentum_ref[i] = momentum
        hydrogen_ref[i] = hydrogen


def post_kernel(cells, d_ref, density_ref, momentum_ref, hydrogen_ref, depth_prev_ref,
                depth_next_ref, parts_ref, weight_ref, plane_ref, line_ref, density_out,
                momentum_out, hydrogen_out, buffer_ref, sem):
    size_x, size_y, size_z = d_ref.shape
    send_density = pltpu.make_async_copy(density_ref, density_out, sem.at[2])
    send_density.start()
    lane = lanes_of((size_y, size_z))
    spot = lane % HALO
    late = (lane // HALO) % 2 == 1
    edge = jnp.where(late, depth_prev_ref[...], depth_next_ref[...])
    low_side = SECOND_COEFFS[3] * edge
    high_side = low_side
    for j in (3, 2, 1):
        w = SECOND_COEFFS[j - 1]
        low_side = low_side + jnp.where(spot < j, w * pltpu.roll(edge, size_z - HALO + j, 1), 0.0)
        high_side = high_side + jnp.where(
            spot >= HALO - j, w * pltpu.roll(edge, HALO - j, 1), 0.0)
    edge = jnp.where(late, low_side, high_side)
    rim = (lane < HALO) | (lane >= size_z - HALO)

    def depth_part(f, i):
        at = 2 * HALO * (f * size_x + i)
        return jnp.where(rim, pltpu.roll(edge, (2 * size_z - HALO - at) % size_z, 1), 0.0)

    for i in range(size_x):
        buffer_ref[0, i] = hydrogen_ref[i] + DIFFUSIVITY * depth_part(1, i)
    send_hydrogen = pltpu.make_async_copy(buffer_ref.at[0], hydrogen_out, sem.at[0])
    send_hydrogen.start()

    parts = [parts_ref[n] for n in range(parts_ref.shape[0])]
    while len(parts) > 1:
        half = len(parts) // 2
        parts = [a + b for a, b in zip(parts[:half], parts[half:])] + parts[2 * half:]
    total = parts[0] * (1.0 / cells)
    quad = lanes_of((4, 128)) // 32
    other = swap64(total)
    waves = jnp.where(quad == 3, -total, total) + jnp.where(quad == 0, -other, other)
    coef = weight_ref[...] * waves
    energy = jnp.sum(jnp.sum(coef * waves, axis=1, keepdims=True), axis=0, keepdims=True)
    other = swap64(coef)
    spec = jnp.where(quad == 3, -coef, coef) + jnp.where(quad == 2, -other, other)
    spec = jnp.concatenate([jnp.where(quad < 2, spec, 0.0), jnp.where(quad < 2, 0.0, spec)], 0)
    mid = fold(jnp.dot(stacked_rows(spec), plane_ref[...], preferred_element_type=jnp.float32))
    high, middle, rest = split(mid)
    mid = jnp.concatenate([high, high, high, middle, middle, rest], 0).astype(jnp.bfloat16)
    low = lax.dot_general(mid, line_ref[...], (((0,), (0,)), ((), ())),
                          preferred_element_type=jnp.float32)
    scale = 2.0 * FORCE_POWER / (energy + ENERGY_EPS)
    force = (low * scale).reshape(size_x, size_y, size_z)
    for i in range(size_x):
        part = momentum_ref[i] + VISCOSITY * depth_part(0, i)
        buffer_ref[1, i] = part + d_ref[i] * force[i]
    send_momentum = pltpu.make_async_copy(buffer_ref.at[1], momentum_out, sem.at[1])
    send_momentum.start()
    send_density.wait()
    send_hydrogen.wait()
    send_momentum.wait()


VMEM_SPEC = pl.BlockSpec(memory_space=pltpu.VMEM)
ANY_SPEC = pl.BlockSpec(memory_space=pl.ANY)


def in_vmem(*args):
    return [pltpu.with_memory_space_constraint(a, pltpu.VMEM) for a in args]


def shift(x, axis, step):
    size = lax.axis_size(axis)
    return lax.ppermute(x, axis, [(i, (i + step) % size) for i in range(size)])


def per_device(density, momentum, hydrogen, forced_modes):
    size_x, size_y, size_z = density.shape
    counts = tuple(lax.axis_size(a) for a in AXES)
    devices = math.prod(counts)
    gather = devices <= 64
    slots = devices if gather else 1
    full = tuple(n * c for n, c in zip(density.shape, counts))
    plane = jnp.asarray(plane_tables(density.shape, counts))
    line = line_tables(size_z, counts[2])
    deep = deep_tables(line)
    f32 = jnp.float32
    sources = (density, momentum, jnp.asarray(line), plane, hydrogen, deep, forced_modes.T)
    kept = [pltpu.VMEM(a.shape[1:] if n in (3, 5) else a.shape, a.dtype)
            for n, a in enumerate(sources) if n != 2]
    block = jax.ShapeDtypeStruct(density.shape, f32)
    block_vmem = pltpu.VMEM(density.shape, f32)
    end = pltpu.VMEM((3, HALO, size_y, size_z), f32)
    outs = pl.pallas_call(
        functools.partial(pre_kernel, slots),
        in_specs=[ANY_SPEC] * 7,
        out_specs=[VMEM_SPEC] * 6 + [ANY_SPEC] + [VMEM_SPEC] * 4,
        out_shape=kept + [
            jax.ShapeDtypeStruct((slots, 4, 128), f32), end, end,
            pltpu.VMEM((2, size_x, 2 * HALO, size_z), f32), pltpu.VMEM((size_y, 128), f32)],
        scratch_shapes=[pltpu.VMEM(line.shape[1:], f32), pltpu.VMEM((slots, 4, 128), f32),
                        pltpu.SemaphoreType.DMA((7,)),
                        pltpu.SemaphoreType.DMA],
    )(*sources)
    density, momentum, plane, hydrogen, deep, modes = outs[:6]
    parts, low, high, side, depth = outs[6:]
    if gather:
        parts = lax.all_to_all(parts, AXES, 0, 0)
    else:
        parts = lax.psum(parts, AXES)
    depth_next = shift(depth, "gz", -1)
    depth_prev = depth_next if counts[2] == 2 else shift(depth, "gz", 1)
    after = shift(low, "gx", -1)
    before = shift(high, "gx", 1)
    side_next = shift(side, "gy", -1)
    side_prev = side_next if counts[1] == 2 else shift(side, "gy", 1)
    pad = pltpu.VMEM((2, size_x, 16 + size_y, size_z), f32)
    own = pl.pallas_call(
        local_kernel,
        in_specs=[VMEM_SPEC] * 5,
        out_specs=[VMEM_SPEC] * 5,
        out_shape=[block_vmem] * 3 + [pltpu.VMEM((4, 128), f32),
                                      pltpu.VMEM((384, size_x * size_y), jnp.bfloat16)],
        scratch_shapes=[pad],
    )(*in_vmem(density, momentum, hydrogen, modes, plane))
    weight, plane = own[3:]
    rates = pl.pallas_call(
        edge_kernel,
        in_specs=[VMEM_SPEC] * 7,
        out_specs=[VMEM_SPEC] * 3,
        out_shape=[block_vmem] * 3,
        scratch_shapes=[pad],
    )(*in_vmem(*own[:3], before, after, side_prev, side_next))
    return tuple(pl.pallas_call(
        functools.partial(post_kernel, float(math.prod(full))),
        in_specs=[VMEM_SPEC] * 10,
        out_specs=[ANY_SPEC] * 3,
        out_shape=[block] * 3,
        scratch_shapes=[pltpu.VMEM((2,) + block.shape, f32), pltpu.SemaphoreType.DMA((3,))],
    )(*in_vmem(density, *rates, depth_prev, depth_next, parts, weight, plane, deep)))


def solution(mesh):
    in_specs = (P("gx", "gy", "gz"), P("gx", "gy", "gz"), P("gx", "gy", "gz"), P())
    out_specs = (P("gx", "gy", "gz"), P("gx", "gy", "gz"), P("gx", "gy", "gz"))
    return jax.shard_map(
        per_device, mesh=mesh, in_specs=in_specs, out_specs=out_specs, check_vma=False
    )
```
